512 devices in a mesh: ctx: 64 (over y, z), head: 8 (over x, core).
Axes of the slice: x: 4, y: 4, z: 16, core: 2. Of those that a mesh axis runs over, the one named last changes fastest.
Arguments:
- queries: bfloat16 [32768, 16, 128], P('ctx', 'head'), may hold values from -130 to 130, as said below
- values: bfloat16 [32768, 16, 128], P('ctx', 'head'), may hold values from -6 to 6
- codes: int32 [32768, 16], P('ctx', 'head'), may hold values from 0 to 511
- codebook: bfloat16 [16, 512, 128], P('head'), may hold values from -8 to 8, as said below
- out_weight: bfloat16 [2048, 2048], P('head'), may hold values from -0.1875 to 0.1875
Outputs:
- mixed: bfloat16 [32768, 2048], P('ctx', 'head')
The draws below stay inside these ranges and needn't reach their ends.
Inputs may be any that keep to these rules, and one draw needn't show every extreme that they name: `queries`: every entry has magnitude at most 130. `codebook`: every entry has magnitude at most 8.
All inputs are finite; a program needn't handle non-finite values.
Results may differ from the reference program's by a relative error of at most 0.0066.
Values may be sent and summed in bfloat16 or wider, within the bound.
A program may use at most 64 MiB of HBM per device.

```python
import jax
import jax.numpy as jnp
from jax import lax

D = 2048
HEADS = 16
DH = 128
CODES = 512
BLOCK = 512
TOKENS = 32768


def shared_codebook(key):
    base = jax.random.truncated_normal(jax.random.fold_in(key, 11), -6.0, 6.0, (HEADS, CODES, DH), jnp.float32)
    return base


def draw_codebook(key, part):
    return shared_codebook(key).astype(jnp.bfloat16)


def draw_queries(key, part):
    drawn = jax.random.truncated_normal(jax.random.fold_in(key, 21), -6.0, 6.0, (TOKENS, HEADS, DH), jnp.float32)
    return drawn.astype(jnp.bfloat16)


def set_ends(values, rng, smallest, high):
    extent = values.shape
    spot = [jax.random.randint(jax.random.fold_in(rng, axis), (), 0, extent[axis]) for axis in range(len(extent))]
    values = values.at[tuple(spot)].set(smallest)
    longest = extent.index(max(extent))
    spot[longest] = (spot[longest] + 1) % extent[longest]
    return values.at[tuple(spot)].set(high)


def with_spikes(result, rng, source, target, parts, factor):
    owner, partner = [(jnp.arange(result.shape[dim]) // (result.shape[dim] // parts)).reshape([-1 if axis == dim else 1 for axis in range(result.ndim)]) for dim in (source, target)]
    chosen = jax.random.permutation(rng, parts)[partner]
    strong = (owner == chosen) | (owner == (partner + parts // 2) % parts)
    return jnp.where(strong, factor * result, result)


def level_of(own_key, extent, split, smallest, high):
    level, own = 1.0, jax.random.fold_in(own_key, 6)
    for axis_at, blocks in split:
        heights = jnp.exp(jax.random.uniform(jax.random.fold_in(own, axis_at), (blocks,), jnp.float32, smallest / len(split), high / len(split)))
        level = level * jnp.repeat(heights, extent[axis_at] // blocks).reshape([-1 if axis == axis_at else 1 for axis in range(len(extent))])
    return level


def gaussian(rng, dims, scale, most, shards=(), dtype=jnp.bfloat16):
    result = scale * jax.random.normal(rng, dims, jnp.float32)
    if shards:
        result = result * level_of(rng, dims, shards, -0.22, 0.18)
    return jnp.clip(result, -most, most).astype(dtype)


def gaussian_with(key, shape, deviation, reach, pieces, heavy, kind=jnp.bfloat16):
    values = deviation * jax.random.normal(key, shape, jnp.float32)
    if pieces:
        values = values * level_of(key, shape, pieces, -0.22, 0.18)
    return jnp.clip(with_spikes(values, jax.random.fold_in(key, 3), *heavy), -reach, reach).astype(kind)


def setup_inputs(seed: int = 0) -> dict:
    key_list = jax.random.split(jax.random.key(seed), 6)
    queries = draw_queries(jax.random.fold_in(key_list[5], 71), 0)
    values = gaussian(key_list[1], (TOKENS, HEADS, DH), 1.0, 6.0, ((0, 64), (1, 8)))
    codes = set_ends(jax.random.randint(key_list[2], (TOKENS, HEADS), 0, CODES), jax.random.fold_in(key_list[2], 1), 0, CODES - 1).astype(jnp.int32)
    codebook = draw_codebook(jax.random.fold_in(key_list[5], 71), 0)
    out_weight = gaussian_with(key_list[4], (HEADS * DH, D), (HEADS * DH) ** -0.5, 0.1875, ((0, 8),), (0, 1, 8, 2.0))
    return dict(queries=queries, values=values, codes=codes, codebook=codebook, out_weight=out_weight)


def attend(query, cur_keys, cur_values, prev_keys, prev_values, live, book, cache_sum, cache_count):
    scale = query.shape[-1] ** -0.5
    code_scores = jnp.dot(query, book.T, preferred_element_type=jnp.float32) * scale
    cur_scores = jnp.dot(query, cur_keys.T, preferred_element_type=jnp.float32) * scale
    prev_scores = jnp.dot(query, prev_keys.T, preferred_element_type=jnp.float32) * scale
    rows = lax.broadcasted_iota(jnp.int32, cur_scores.shape, 0)
    cols = lax.broadcasted_iota(jnp.int32, cur_scores.shape, 1)
    causal = rows >= cols
    present = (cache_count > 0.0)[None, :]
    top = jnp.max(jnp.where(causal, cur_scores, -jnp.inf), axis=1)
    top = jnp.maximum(top, jnp.max(jnp.where(live, prev_scores, -jnp.inf), axis=1))
    top = jnp.maximum(top, jnp.max(jnp.where(present, code_scores, -jnp.inf), axis=1))
    top = top[:, None]
    cur_weight = jnp.where(causal, jnp.exp(cur_scores - top), 0.0)
    prev_weight = jnp.where(live, jnp.exp(prev_scores - top), 0.0)
    code_weight = jnp.where(present, jnp.exp(code_scores - top), 0.0)
    denom = jnp.sum(cur_weight, axis=1) + jnp.sum(prev_weight, axis=1) + jnp.sum(code_weight * cache_count[None, :], axis=1)
    numer = jnp.dot(cur_weight.astype(jnp.bfloat16), cur_values, preferred_element_type=jnp.float32)
    numer = numer + jnp.dot(prev_weight.astype(jnp.bfloat16), prev_values, preferred_element_type=jnp.float32)
    numer = numer + jnp.dot(code_weight, cache_sum, precision=lax.Precision.HIGHEST)
    return (numer / denom[:, None]).astype(jnp.bfloat16)


def reference(queries, values, codes, codebook, out_weight):
    heads = codebook.shape[0]
    width = codebook.shape[2]
    ncodes = codebook.shape[1]
    nblocks = TOKENS // BLOCK
    keys = jax.vmap(lambda book, index: book[index], in_axes=(0, 1), out_axes=1)(codebook, codes)
    query_blocks = queries.reshape(nblocks, BLOCK, heads, width)
    key_blocks = keys.reshape(nblocks, BLOCK, heads, width)
    value_blocks = values.reshape(nblocks, BLOCK, heads, width)
    code_blocks = codes.reshape(nblocks, BLOCK, heads)
    table = lax.broadcasted_iota(jnp.int32, (1, 1, ncodes), 2)

    def step(carry, block):
        cache_sum, cache_count, pend_sum, pend_count, prev_keys, prev_values, live = carry
        query, key, value, index = block
        attended = jax.vmap(attend, in_axes=(1, 1, 1, 1, 1, None, 0, 0, 0), out_axes=1)(
            query, key, value, prev_keys, prev_values, live, codebook, cache_sum, cache_count)
        onehot = (index[:, :, None] == table).astype(jnp.float32)
        sums = jnp.einsum("ths,thd->hsd", onehot, value.astype(jnp.float32), precision=lax.Precision.HIGHEST)
        counts = jnp.sum(onehot, axis=0)
        carry = (cache_sum + pend_sum, cache_count + pend_count, sums, counts, key, value, jnp.array(True))
        return carry, attended

    zero_sum = jnp.zeros((heads, ncodes, width), jnp.float32)
    zero_count = jnp.zeros((heads, ncodes), jnp.float32)
    zero_block = jnp.zeros((BLOCK, heads, width), jnp.bfloat16)
    start = (zero_sum, zero_count, zero_sum, zero_count, zero_block, zero_block, jnp.array(False))
    final, outputs = lax.scan(step, start, (query_blocks, key_blocks, value_blocks, code_blocks))
    attended = outputs.reshape(TOKENS, heads * width)
    return jnp.dot(attended, out_weight, preferred_element_type=jnp.float32).astype(jnp.bfloat16)
```

```python
import functools

import jax
import jax.numpy as jnp
from jax import lax
from jax.experimental import pallas as pl
from jax.experimental.pallas import tpu as pltpu
from jax.sharding import Mesh
from jax.sharding import PartitionSpec as P

MESH = pl.DeviceIdType.MESH
CTX = ("y", "z")
HEAD = ("x", "c")
F32 = jnp.float32
BF16 = jnp.bfloat16
NEG = float("-inf")


def dot_nt(a, b):
    return lax.dot_general(a, b, (((1,), (1,)), ((), ())), preferred_element_type=F32)


def dot_nn(a, b, precision=None):
    return lax.dot_general(
        a, b, (((1,), (0,)), ((), ())), precision=precision, preferred_element_type=F32
    )


def wait_bytes(ref, sem):
    pltpu.make_async_copy(ref, ref, sem).wait()


def kernel(
    q_ref, v_ref, col_ref, row_ref, book_ref, w_ref, out_ref,
    sums, raw, tot_s, tot_r, pre_s, cache,
    csums, craw, ctot_s, ctot_r, cpre_s, ccache,
    code_sc, fw, aloc, stat, gath, wcol,
    z_send, z_recv, y_send, y_recv, w_send, w_recv, w_local, g_send, g_recv,
    *, ny, nz, nx,
):
    heads, tokens, width = q_ref.shape
    ncodes = book_ref.shape[1]
    sl = ncodes // nz
    half = tokens // 2
    cols = out_ref.shape[1]
    y, z, x, c = (lax.axis_index(name) for name in ("y", "z", "x", "c"))

    def far_first(j):
        step = (j + 1) // 2
        sign = 1 - 2 * lax.rem(j, 2)
        return lax.rem(z + nz // 2 + sign * step + nz, nz)

    def x_at(d):
        return lax.rem(x + d, nx)

    barrier = pltpu.get_barrier_semaphore()

    def greet(j, carry):
        pl.semaphore_signal(barrier, inc=1, device_id={"z": far_first(j)}, device_id_type=MESH)
        return carry

    lax.fori_loop(0, nz - 1, greet, 0)
    for d in range(1, ny):
        there = {"y": lax.rem(y + d, ny)}
        pl.semaphore_signal(barrier, inc=1, device_id=there, device_id_type=MESH)
    peers = [(dx, dc) for dx in range(nx) for dc in range(2)][1:]
    for dx, dc in peers:
        there = {"x": x_at(dx), "c": lax.rem(c + dc, 2)}
        pl.semaphore_signal(barrier, inc=1, device_id=there, device_id_type=MESH)

    for h in range(heads):
        onehot_t = (
            lax.broadcasted_iota(jnp.int32, (ncodes, tokens), 0) == row_ref[h : h + 1, :]
        ).astype(BF16)
        both = jnp.concatenate([v_ref[h], jnp.ones((tokens, width), BF16)], axis=1)
        summed = dot_nn(onehot_t, both)
        sums[h] = summed[:, :width].astype(BF16).reshape(nz, sl, width)
        lane = lax.broadcasted_iota(jnp.int32, (ncodes, width), 1)
        code = lax.broadcasted_iota(jnp.int32, (ncodes, width), 0)
        mine = jnp.where(lane == h * sl + lax.rem(code, sl), summed[:, width:], 0.0)
        counted = jnp.sum(mine.reshape(nz, sl, width), axis=1)
        if h == 0:
            counts = counted
        else:
            counts = counts + counted
    csums[...] = counts.reshape(nz, 1, width)

    def block_scores(h):
        onehot = (
            lax.broadcasted_iota(jnp.int32, (tokens, ncodes), 1) == col_ref[:, h : h + 1]
        ).astype(BF16)
        keys = dot_nn(onehot, book_ref[h]).astype(BF16)
        scale = width ** (-0.5)
        code_sc[h] = dot_nt(q_ref[h], book_ref[h]) * scale
        scores = dot_nt(q_ref[h], keys) * scale
        rows = lax.broadcasted_iota(jnp.int32, (tokens, tokens), 0)
        ends = lax.broadcasted_iota(jnp.int32, (tokens, tokens), 1)
        scores = jnp.where(rows >= ends, scores, NEG)
        top = jnp.max(scores, axis=1, keepdims=True)
        weights = jnp.exp(scores - top)
        aloc[h] = dot_nn(weights.astype(BF16), v_ref[h])
        stat[h, 0] = top
        stat[h, 1] = jnp.sum(weights, axis=1, keepdims=True)

    pl.semaphore_wait(barrier, nz - 1 + ny - 1 + len(peers))

    def z_push(source, target, chunk):
        def push(j, carry):
            there = far_first(j)
            pltpu.make_async_remote_copy(
                src_ref=source.at[there],
                dst_ref=target.at[z],
                send_sem=z_send.at[chunk],
                recv_sem=z_recv.at[chunk],
                device_id={"z": there},
                device_id_type=MESH,
            ).start()
            return carry

        lax.fori_loop(0, nz - 1, push, 0)
        target[z] = source[z]

    z_push(csums, craw, 0)
    for h in range(heads):
        z_push(sums.at[h], raw.at[h], 1 + h)

    def w_slice(dx, dc):
        owner = x_at(dx) * 2 + lax.rem(c + dc, 2)
        return w_ref.at[:, pl.ds(pl.multiple_of(owner * cols, cols), cols)]

    own_w = pltpu.make_async_copy(w_slice(0, 0), wcol.at[0, 0], w_local)
    own_w.start()
    w_copies = []
    for dx, dc in peers:
        copy = pltpu.make_async_remote_copy(
            src_ref=w_slice(dx, dc),
            dst_ref=wcol.at[(nx - dx) % nx, dc],
            send_sem=w_send.at[dx, dc],
            recv_sem=w_recv.at[(nx - dx) % nx, dc],
            device_id={"x": x_at(dx), "c": lax.rem(c + dc, 2)},
            device_id_type=MESH,
        )
        copy.start()
        w_copies.append(copy)

    for h in range(heads):
        block_scores(h)

    def scan_z(read, chunk, received, store_total, store):
        wait_bytes(received, z_recv.at[chunk])
        before = []
        so_far = None
        for n in range(nz):
            part = read(n)
            before.append(so_far)
            so_far = part if so_far is None else so_far + part
        store_total(so_far)
        for n in range(nz):
            store(n, jnp.zeros_like(so_far) if before[n] is None else before[n])

    def y_push(source, target, chunk):
        for d in range(1, ny):
            pltpu.make_async_remote_copy(
                src_ref=source,
                dst_ref=target.at[ny - d],
                send_sem=y_send.at[chunk],
                recv_sem=y_recv.at[chunk],
                device_id={"y": lax.rem(y + d, ny)},
                device_id_type=MESH,
            ).start()

    def earlier_rows(target, chunk):
        wait_bytes(target.at[pl.ds(1, ny - 1)], y_recv.at[chunk])
        total = None
        for d in range(1, ny):
            part = jnp.where(y + d >= ny, target[d].astype(F32), 0.0)
            total = part if total is None else total + part
        return total

    wait_bytes(craw.at[pl.ds(0, nz - 1)], z_recv.at[0])
    before, so_far = [], jnp.zeros((1, width), F32)
    for n in range(nz):
        before.append(so_far)
        so_far = so_far + craw[n]
    ctot_s[...] = so_far
    y_push(ctot_s, ctot_r, 0)
    above = earlier_rows(ctot_r, 0)
    for n in range(nz):
        cpre_s[n] = before[n] + above
    z_push(cpre_s, ccache, 3)

    def head_prefix(h):
        wait_bytes(raw.at[h, pl.ds(0, nz - 1)], z_recv.at[1 + h])
        before, so_far = [], jnp.zeros((sl, width), F32)
        for n in range(nz):
            before.append(so_far)
            so_far = so_far + raw[h, n].astype(F32)
        tot_s[h] = so_far.astype(BF16)
        y_push(tot_s.at[h], tot_r.at[h], 1 + h)
        above = earlier_rows(tot_r.at[h], 1 + h)
        for n in range(nz):
            pre_s[h, n] = (before[n] + above).astype(BF16)
        z_push(pre_s.at[h], cache.at[h], 4 + h)

    for h in range(heads):
        head_prefix(h)

    wait_bytes(ccache.at[pl.ds(0, nz - 1)], z_recv.at[3])
    found = ccache[...].reshape(nz, width)
    for h in range(heads):
        lane = lax.broadcasted_iota(jnp.int32, (width, ncodes), 0)
        code = lax.broadcasted_iota(jnp.int32, (width, ncodes), 1)
        pick = (lane == h * sl + lax.rem(code, sl)).astype(F32)
        spread = dot_nn(found, pick, lax.Precision.HIGHEST)
        group = lax.broadcasted_iota(jnp.int32, (nz, ncodes), 0)
        where = lax.broadcasted_iota(jnp.int32, (nz, ncodes), 1) // sl
        count = jnp.sum(jnp.where(group == where, spread, 0.0), axis=0, keepdims=True)
        scores = jnp.where(count > 0.0, code_sc[h], NEG)
        top = jnp.maximum(stat[h, 0], jnp.max(scores, axis=1, keepdims=True))
        weights = jnp.exp(scores - top)
        shift = jnp.exp(stat[h, 0] - top)
        den = stat[h, 1] * shift + jnp.sum(weights * count, axis=1, keepdims=True)
        inverse = 1.0 / den
        fw[h] = (weights * inverse).astype(BF16)
        aloc[h] = aloc[h] * (shift * inverse)

    def g_copy(h, r, slot, dx, dc, number):
        sx, sc = slot
        rows = pl.ds(r * half, half)
        return pltpu.make_async_remote_copy(
            src_ref=gath.at[h, sx, sc, rows],
            dst_ref=gath.at[h, (sx - dx) % nx, (sc + dc) % 2, rows],
            send_sem=g_send.at[h, number],
            recv_sem=g_recv.at[h, (sx - dx) % nx, (sc + dc) % 2, r],
            device_id={"x": x_at(dx), "c": lax.rem(c + dc, 2)},
            device_id_type=MESH,
        )

    right, left = 1, nx - 1
    sent = []

    def send(h, r, slot, dx, dc):
        number = sum(1 for other, _ in sent if other == h)
        copy = g_copy(h, r, slot, dx, dc, number)
        copy.start()
        sent.append((h, copy))

    def landed(h, r, slot):
        sx, sc = slot
        ref = gath.at[h, sx, sc, pl.ds(r * half, half)]
        wait_bytes(ref, g_recv.at[h, sx, sc, r])

    def finish(h):
        wait_bytes(cache.at[h, pl.ds(0, nz - 1)], z_recv.at[4 + h])
        table = cache[h].reshape(ncodes, width)
        gath[h, 0, 0] = (aloc[h] + dot_nn(fw[h], table)).astype(BF16)
        for r in range(2):
            send(h, r, (0, 0), right, 0)
            send(h, 1 - r, (0, 0), left, 0)
        for r in range(2):
            send(h, r, (0, 0), 0, 1)

    def relay(h):
        landed(h, 0, (left, 0))
        send(h, 0, (left, 0), right, 0)
        send(h, 0, (left, 0), 0, 1)
        landed(h, 1, (right, 0))
        send(h, 1, (right, 0), left, 0)
        send(h, 1, (right, 0), 0, 1)
        landed(h, 1, (left, 0))
        send(h, 1, (left, 0), 0, 1)
        landed(h, 0, (right, 0))
        send(h, 0, (right, 0), 0, 1)
        for r in range(2):
            landed(h, r, (2, 0))
            send(h, r, (2, 0), 0, 1)

    def project(h, slots, total):
        for sx, sc in slots:
            part = dot_nn(gath[h, sx, sc], wcol[sx, sc, h * width : (h + 1) * width, :])
            total = part if total is None else total + part
        return total

    direct = [(0, 0), (left, 0), (right, 0), (2, 0)]
    other = [(0, 1), (left, 1), (right, 1), (2, 1)]

    finish(0)
    relay(0)
    finish(1)
    own_w.wait()
    for copy in w_copies:
        copy.wait()
    relay(1)
    total = project(0, direct, None)
    for slot in other:
        for r in range(2):
            landed(0, r, slot)
    total = project(0, other, total)
    total = project(1, direct, total)
    for slot in other:
        for r in range(2):
            landed(1, r, slot)
    total = project(1, other, total)
    out_ref[...] = total.astype(BF16)

    for _, copy in sent:
        copy.wait_send()
    for chunk, ref in ((0, csums), (1, sums.at[0]), (2, sums.at[1])):
        wait_bytes(ref.at[pl.ds(0, nz - 1)], z_send.at[chunk])
    for chunk, ref in ((3, cpre_s), (4, pre_s.at[0]), (5, pre_s.at[1])):
        wait_bytes(ref.at[pl.ds(0, nz - 1)], z_send.at[chunk])
    for chunk, ref in ((0, ctot_r), (1, tot_r.at[0]), (2, tot_r.at[1])):
        wait_bytes(ref.at[pl.ds(1, ny - 1)], y_send.at[chunk])


def on_device(queries, values, codes, codebook, out_weight, *, ny, nz, nx):
    tokens, heads, width = queries.shape
    ncodes = codebook.shape[1]
    sl = ncodes // nz
    cols = out_weight.shape[1] // (nx * 2)
    depth = out_weight.shape[0]
    vmem = pl.BlockSpec(memory_space=pltpu.VMEM)
    scratch = [
        pltpu.VMEM((heads, nz, sl, width), BF16),
        pltpu.VMEM((heads, nz, sl, width), BF16),
        pltpu.VMEM((heads, sl, width), BF16),
        pltpu.VMEM((heads, ny, sl, width), BF16),
        pltpu.VMEM((heads, nz, sl, width), BF16),
        pltpu.VMEM((heads, nz, sl, width), BF16),
        pltpu.VMEM((nz, 1, width), F32),
        pltpu.VMEM((nz, 1, width), F32),
        pltpu.VMEM((1, width), F32),
        pltpu.VMEM((ny, 1, width), F32),
        pltpu.VMEM((nz, 1, width), F32),
        pltpu.VMEM((nz, 1, width), F32),
        pltpu.VMEM((heads, tokens, ncodes), F32),
        pltpu.VMEM((heads, tokens, ncodes), BF16),
        pltpu.VMEM((heads, tokens, width), F32),
        pltpu.VMEM((heads, 2, tokens, 1), F32),
        pltpu.VMEM((heads, nx, 2, tokens, width), BF16),
        pltpu.VMEM((nx, 2, depth, cols), BF16),
        pltpu.SemaphoreType.DMA((6,)),
        pltpu.SemaphoreType.DMA((6,)),
        pltpu.SemaphoreType.DMA((3,)),
        pltpu.SemaphoreType.DMA((3,)),
        pltpu.SemaphoreType.DMA((nx, 2)),
        pltpu.SemaphoreType.DMA((nx, 2)),
        pltpu.SemaphoreType.DMA,
        pltpu.SemaphoreType.DMA((heads, 16)),
        pltpu.SemaphoreType.DMA((heads, nx, 2, 2)),
    ]
    return pl.pallas_call(
        functools.partial(kernel, ny=ny, nz=nz, nx=nx),
        out_shape=jax.ShapeDtypeStruct((tokens, cols), BF16),
        in_specs=[vmem] * 5 + [pl.BlockSpec(memory_space=pl.ANY)],
        out_specs=vmem,
        scratch_shapes=scratch,
        compiler_params=pltpu.CompilerParams(collective_id=0, has_side_effects=True),
        name="vq_layer",
    )(
        jnp.swapaxes(queries, 0, 1),
        jnp.swapaxes(values, 0, 1),
        codes,
        codes.T,
        codebook,
        out_weight,
    )


def layer(mesh, ny, nz, nx):
    finer = Mesh(mesh.devices.reshape(ny, nz, nx, 2), ("y", "z", "x", "c"))
    placed = (
        P(CTX, HEAD, None),
        P(CTX, HEAD, None),
        P(CTX, HEAD),
        P(HEAD, None, None),
        P(HEAD, None),
    )
    return jax.shard_map(
        functools.partial(on_device, ny=ny, nz=nz, nx=nx),
        mesh=finer,
        in_specs=placed,
        out_specs=P(CTX, HEAD),
        check_vma=False,
    )


def solution(mesh):
    return layer(mesh, 4, 16, 4)
```

```python
import functools

import jax
import jax.numpy as jnp
from jax import lax
from jax.experimental import pallas as pl
from jax.experimental.pallas import tpu as pltpu
from jax.sharding import Mesh
from jax.sharding import PartitionSpec as P

MESH = pl.DeviceIdType.MESH
CTX = ("y", "z")
HEAD = ("x", "c")
F32 = jnp.float32
BF16 = jnp.bfloat16
NEG = float("-inf")


def dot_nt(a, b):
    return lax.dot_general(a, b, (((1,), (1,)), ((), ())), preferred_element_type=F32)


def dot_nn(a, b, precision=None):
    return lax.dot_general(
        a, b, (((1,), (0,)), ((), ())), precision=precision, preferred_element_type=F32
    )


def dot_tn(a, b):
    return lax.dot_general(a, b, (((0,), (0,)), ((), ())), preferred_element_type=F32)


def wait_bytes(ref, sem):
    pltpu.make_async_copy(ref, ref, sem).wait()


def kernel(
    q_ref, v_ref, row_ref, book_ref, w_ref, out_ref,
    qin, vin, codes, book, split, vals, qs,
    sums, raw, tot_s, tot_r, pre_s, cache,
    csums, craw, ctot_s, ctot_r, cpre_s, ccache,
    code_sc, fw, aloc, stat, gath, wcol, acc,
    in_sem, z_send, z_recv, y_send, y_recv, w_send, w_recv, w_local, g_send, g_recv,
    *, ny, nz, nx, nch,
):
    heads, ncodes, width = book_ref.shape
    tokens = q_ref.shape[0] // heads
    sl = ncodes // nz
    part = tokens // nch
    cols = out_ref.shape[1]
    y, z, x, c = (lax.axis_index(name) for name in ("y", "z", "x", "c"))
    scope = jax.named_scope

    def far_first(j):
        step = (j + 1) // 2
        sign = 1 - 2 * lax.rem(j, 2)
        return lax.rem(z + nz // 2 + sign * step + nz, nz)

    def x_at(d):
        return lax.rem(x + d, nx)

    barrier = pltpu.get_barrier_semaphore()

    def greet(j, carry):
        pl.semaphore_signal(barrier, inc=1, device_id={"z": far_first(j)}, device_id_type=MESH)
        return carry

    lax.fori_loop(0, nz - 1, greet, 0)
    for d in range(1, ny):
        there = {"y": lax.rem(y + d, ny)}
        pl.semaphore_signal(barrier, inc=1, device_id=there, device_id_type=MESH)
    peers = [(dx, dc) for dx in range(nx) for dc in range(2)][1:]
    for dx, dc in peers:
        there = {"x": x_at(dx), "c": lax.rem(c + dc, 2)}
        pl.semaphore_signal(barrier, inc=1, device_id=there, device_id_type=MESH)

    loads = []
    for number, (source, target) in enumerate(
        ((row_ref, codes), (v_ref, vin), (book_ref, book), (q_ref, qin))
    ):
        loads.append(pltpu.make_async_copy(source, target, in_sem.at[number]))
        loads[-1].start()

    with scope("load"):
        loads[0].wait()
        loads[1].wait()
    with scope("sums"):
        split[...] = vin[...].astype(F32)
        counts = None
        for h in range(heads):
            vals[h] = split[pl.ds(h, tokens, stride=heads), :].astype(BF16)
            onehot_t = (
                lax.broadcasted_iota(jnp.int32, (ncodes, tokens), 0) == codes[h : h + 1, :]
            ).astype(BF16)
            both = jnp.concatenate([vals[h], jnp.ones((tokens, width), BF16)], axis=1)
            summed = dot_nn(onehot_t, both)
            sums[h] = summed[:, :width].astype(BF16).reshape(nz, sl, width)
            lane = lax.broadcasted_iota(jnp.int32, (ncodes, width), 1)
            code = lax.broadcasted_iota(jnp.int32, (ncodes, width), 0)
            mine = jnp.where(lane == h * sl + lax.rem(code, sl), summed[:, width:], 0.0)
            counted = jnp.sum(mine.reshape(nz, sl, width), axis=1)
            counts = counted if counts is None else counts + counted
        csums[...] = counts.reshape(nz, 1, width)

    def block_scores(h):
        onehot_t = (
            lax.broadcasted_iota(jnp.int32, (ncodes, tokens), 0) == codes[h : h + 1, :]
        ).astype(BF16)
        keys_t = dot_tn(book[h], onehot_t).astype(BF16)
        scale = width ** (-0.5)
        code_sc[h] = dot_nt(qs[h], book[h]) * scale
        scores = dot_nn(qs[h], keys_t) * scale
        rows = lax.broadcasted_iota(jnp.int32, (tokens, tokens), 0)
        ends = lax.broadcasted_iota(jnp.int32, (tokens, tokens), 1)
        scores = jnp.where(rows >= ends, scores, NEG)
        top = jnp.max(scores, axis=1, keepdims=True)
        weights = jnp.exp(scores - top)
        aloc[h] = dot_nn(weights.astype(BF16), vals[h])
        stat[h, 0] = top
        stat[h, 1] = jnp.sum(weights, axis=1, keepdims=True)

    with scope("barrier"):
        pl.semaphore_wait(barrier, nz - 1 + ny - 1 + len(peers))

    def z_push(source, target, chunk):
        def push(j, carry):
            there = far_first(j)
            pltpu.make_async_remote_copy(
                src_ref=source.at[there],
                dst_ref=target.at[z],
                send_sem=z_send.at[chunk],
                recv_sem=z_recv.at[chunk],
                device_id={"z": there},
                device_id_type=MESH,
            ).start()
            return carry

        lax.fori_loop(0, nz - 1, push, 0)
        target[z] = source[z]

    with scope("push_raw"):
        z_push(csums, craw, 0)
        for h in range(heads):
            z_push(sums.at[h], raw.at[h], 1 + h)

    def w_slice(dx, dc):
        owner = x_at(dx) * 2 + lax.rem(c + dc, 2)
        return w_ref.at[:, pl.ds(pl.multiple_of(owner * cols, cols), cols)]

    own_w = pltpu.make_async_copy(w_slice(0, 0), wcol.at[0, 0], w_local)
    own_w.start()
    w_copies = []
    for dx, dc in peers:
        copy = pltpu.make_async_remote_copy(
            src_ref=w_slice(dx, dc),
            dst_ref=wcol.at[(nx - dx) % nx, dc],
            send_sem=w_send.at[dx, dc],
            recv_sem=w_recv.at[(nx - dx) % nx, dc],
            device_id={"x": x_at(dx), "c": lax.rem(c + dc, 2)},
            device_id_type=MESH,
        )
        copy.start()
        w_copies.append(copy)

    with scope("scores"):
        loads[2].wait()
        loads[3].wait()
        split[...] = qin[...].astype(F32)
        for h in range(heads):
            qs[h] = split[pl.ds(h, tokens, stride=heads), :].astype(BF16)
            block_scores(h)

    def y_push(source, target, chunk):
        for d in range(1, ny):
            pltpu.make_async_remote_copy(
                src_ref=source,
                dst_ref=target.at[ny - d],
                send_sem=y_send.at[chunk],
                recv_sem=y_recv.at[chunk],
                device_id={"y": lax.rem(y + d, ny)},
                device_id_type=MESH,
            ).start()

    with scope("wait_craw"):
        wait_bytes(craw.at[pl.ds(0, nz - 1)], z_recv.at[0])
    cbefore, so_far = [], jnp.zeros((1, width), F32)
    for n in range(nz):
        cbefore.append(so_far)
        so_far = so_far + craw[n]
    ctot_s[...] = so_far
    y_push(ctot_s, ctot_r, 0)
    for h in range(heads):
        with scope(f"wait_raw{h}"):
            wait_bytes(raw.at[h, pl.ds(0, nz - 1)], z_recv.at[1 + h])
        so_far = raw[h, 0].astype(F32)
        for n in range(1, nz):
            so_far = so_far + raw[h, n].astype(F32)
        tot_s[h] = so_far.astype(BF16)
    y_push(tot_s, tot_r, 1)

    def earlier_rows(target):
        total = None
        for d in range(1, ny):
            row = jnp.where(y + d >= ny, target(d).astype(F32), 0.0)
            total = row if total is None else total + row
        return total

    with scope("wait_cy"):
        wait_bytes(ctot_r.at[pl.ds(1, ny - 1)], y_recv.at[0])
    above = earlier_rows(lambda d: ctot_r[d])
    for n in range(nz):
        cpre_s[n] = cbefore[n] + above
    z_push(cpre_s, ccache, 3)
    with scope("wait_y"):
        wait_bytes(tot_r.at[pl.ds(1, ny - 1)], y_recv.at[1])
    with scope("prefix"):
        for h in range(heads):
            so_far = earlier_rows(lambda d, h=h: tot_r[d, h])
            for n in range(nz):
                pre_s[h, n] = so_far.astype(BF16)
                so_far = so_far + raw[h, n].astype(F32)
            z_push(pre_s.at[h], cache.at[h], 4 + h)

    with scope("wait_ccache"):
        wait_bytes(ccache.at[pl.ds(0, nz - 1)], z_recv.at[3])

    def code_weights(h):
        lane = lax.broadcasted_iota(jnp.int32, (width, ncodes), 0)
        code = lax.broadcasted_iota(jnp.int32, (width, ncodes), 1)
        pick = (lane == h * sl + lax.rem(code, sl)).astype(F32)
        spread = dot_nn(found, pick, lax.Precision.HIGHEST)
        group = lax.broadcasted_iota(jnp.int32, (nz, ncodes), 0)
        where = lax.broadcasted_iota(jnp.int32, (nz, ncodes), 1) // sl
        count = jnp.sum(jnp.where(group == where, spread, 0.0), axis=0, keepdims=True)
        scores = jnp.where(count > 0.0, code_sc[h], NEG)
        top = jnp.maximum(stat[h, 0], jnp.max(scores, axis=1, keepdims=True))
        weights = jnp.exp(scores - top)
        shift = jnp.exp(stat[h, 0] - top)
        den = stat[h, 1] * shift + jnp.sum(weights * count, axis=1, keepdims=True)
        inverse = 1.0 / den
        fw[h] = (weights * inverse).astype(BF16)
        aloc[h] = aloc[h] * (shift * inverse)

    with scope("weights"):
        found = ccache[...].reshape(nz, width)
        for h in range(heads):
            code_weights(h)

    right, left = 1, nx - 1

    def piece(slot, h, r):
        return gath.at[slot[0], slot[1], pl.ds(r * part, part), pl.ds(h * width, width)]

    copies = []

    def send(h, r, slot, dx, dc):
        there = ((slot[0] - dx) % nx, (slot[1] + dc) % 2)
        copy = pltpu.make_async_remote_copy(
            src_ref=piece(slot, h, r),
            dst_ref=piece(there, h, r),
            send_sem=g_send.at[len(copies)],
            recv_sem=g_recv.at[h, there[0], there[1], r],
            device_id={"x": x_at(dx), "c": lax.rem(c + dc, 2)},
            device_id_type=MESH,
        )
        copy.start()
        copies.append(copy)

    def landed(h, r, slot):
        wait_bytes(piece(slot, h, r), g_recv.at[h, slot[0], slot[1], r])

    low, high = range(nch // 2), range(nch // 2, nch)
    for h in range(heads):
        with scope(f"wait_cache{h}"):
            wait_bytes(cache.at[h, pl.ds(0, nz - 1)], z_recv.at[4 + h])
        table = cache[h].reshape(ncodes, width)
        gath[0, 0, :, h * width : (h + 1) * width] = (aloc[h] + dot_nn(fw[h], table)).astype(BF16)
        for r, s in zip((*low, *high), (*high, *low), strict=True):
            send(h, r, (0, 0), right, 0)
            send(h, s, (0, 0), left, 0)
        for r in range(nch):
            send(h, r, (0, 0), 0, 1)

    def project(slot, first=False):
        add = dot_nn(gath[slot[0], slot[1]], wcol[slot[0], slot[1]])
        acc[...] = add if first else acc[...] + add

    with scope("wait_w"):
        own_w.wait()
        for copy in w_copies:
            copy.wait()
    project((0, 0), True)
    for h in range(heads):
        with scope(f"relay{h}"):
            for r, s in zip(low, high, strict=True):
                landed(h, r, (left, 0))
                send(h, r, (left, 0), right, 0)
                send(h, r, (left, 0), 0, 1)
                landed(h, s, (right, 0))
                send(h, s, (right, 0), left, 0)
                send(h, s, (right, 0), 0, 1)
            for r, s in zip(high, low, strict=True):
                landed(h, r, (left, 0))
                send(h, r, (left, 0), 0, 1)
                landed(h, s, (right, 0))
                send(h, s, (right, 0), 0, 1)
    for h in range(heads):
        with scope(f"across{h}"):
            for r, s in zip(low, high, strict=True):
                landed(h, r, (2, 0))
                send(h, r, (2, 0), 0, 1)
                landed(h, s, (2, 0))
                send(h, s, (2, 0), 0, 1)
    for slot in ((left, 0), (right, 0), (2, 0)):
        project(slot)
    for slot in ((0, 1), (left, 1), (right, 1), (2, 1)):
        with scope("other"):
            for h in range(heads):
                for r in range(nch):
                    landed(h, r, slot)
        project(slot)
    out_ref[...] = acc[...].astype(BF16)

    with scope("tail"):
        for copy in copies:
            copy.wait_send()
        for chunk, ref in ((0, csums), (1, sums.at[0]), (2, sums.at[1])):
            wait_bytes(ref.at[pl.ds(0, nz - 1)], z_send.at[chunk])
        for chunk, ref in ((3, cpre_s), (4, pre_s.at[0]), (5, pre_s.at[1])):
            wait_bytes(ref.at[pl.ds(0, nz - 1)], z_send.at[chunk])
        for chunk, ref in ((0, ctot_r), (1, tot_r)):
            wait_bytes(ref.at[pl.ds(1, ny - 1)], y_send.at[chunk])


def on_device(queries, values, codes, codebook, out_weight, *, ny, nz, nx):
    tokens, heads, width = queries.shape
    ncodes = codebook.shape[1]
    sl = ncodes // nz
    cols = out_weight.shape[1] // (nx * 2)
    depth = out_weight.shape[0]
    nch = 4
    anywhere = pl.BlockSpec(memory_space=pl.ANY)
    ncopies = heads * (3 * nch + nch + 3 * nch)
    scratch = [
        pltpu.VMEM((tokens * heads, width), BF16),
        pltpu.VMEM((tokens * heads, width), BF16),
        pltpu.VMEM((heads, tokens), jnp.int32),
        pltpu.VMEM((heads, ncodes, width), BF16),
        pltpu.VMEM((tokens * heads, width), F32),
        pltpu.VMEM((heads, tokens, width), BF16),
        pltpu.VMEM((heads, tokens, width), BF16),
        pltpu.VMEM((heads, nz, sl, width), BF16),
        pltpu.VMEM((heads, nz, sl, width), BF16),
        pltpu.VMEM((heads, sl, width), BF16),
        pltpu.VMEM((ny, heads, sl, width), BF16),
        pltpu.VMEM((heads, nz, sl, width), BF16),
        pltpu.VMEM((heads, nz, sl, width), BF16),
        pltpu.VMEM((nz, 1, width), F32),
        pltpu.VMEM((nz, 1, width), F32),
        pltpu.VMEM((1, width), F32),
        pltpu.VMEM((ny, 1, width), F32),
        pltpu.VMEM((nz, 1, width), F32),
        pltpu.VMEM((nz, 1, width), F32),
        pltpu.VMEM((heads, tokens, ncodes), F32),
        pltpu.VMEM((heads, tokens, ncodes), BF16),
        pltpu.VMEM((heads, tokens, width), F32),
        pltpu.VMEM((heads, 2, tokens, 1), F32),
        pltpu.VMEM((nx, 2, tokens, depth), BF16),
        pltpu.VMEM((nx, 2, depth, cols), BF16),
        pltpu.VMEM((tokens, cols), F32),
        pltpu.SemaphoreType.DMA((4,)),
        pltpu.SemaphoreType.DMA((6,)),
        pltpu.SemaphoreType.DMA((6,)),
        pltpu.SemaphoreType.DMA((2,)),
        pltpu.SemaphoreType.DMA((2,)),
        pltpu.SemaphoreType.DMA((nx, 2)),
        pltpu.SemaphoreType.DMA((nx, 2)),
        pltpu.SemaphoreType.DMA,
        pltpu.SemaphoreType.DMA((ncopies,)),
        pltpu.SemaphoreType.DMA((heads, nx, 2, nch)),
    ]
    return pl.pallas_call(
        functools.partial(kernel, ny=ny, nz=nz, nx=nx, nch=nch),
        out_shape=pltpu.VMEM((tokens, cols), BF16),
        in_specs=[anywhere] * 5,
        out_specs=pl.BlockSpec(memory_space=pltpu.VMEM),
        scratch_shapes=scratch,
        compiler_params=pltpu.CompilerParams(collective_id=0, has_side_effects=True),
        name="vq_layer",
    )(
        queries.reshape(tokens * heads, width),
        values.reshape(tokens * heads, width),
        codes.T,
        codebook,
        out_weight,
    )


def layer(mesh, ny, nz, nx):
    finer = Mesh(mesh.devices.reshape(ny, nz, nx, 2), ("y", "z", "x", "c"))
    placed = (
        P(CTX, HEAD, None),
        P(CTX, HEAD, None),
        P(CTX, HEAD),
        P(HEAD, None, None),
        P(HEAD, None),
    )
    return jax.shard_map(
        functools.partial(on_device, ny=ny, nz=nz, nx=nx),
        mesh=finer,
        in_specs=placed,
        out_specs=P(CTX, HEAD),
        check_vma=False,
    )


def solution(mesh):
    return layer(mesh, 4, 16, 4)
```

```python
import functools

import jax
import jax.numpy as jnp
from jax import lax
from jax.experimental import pallas as pl
from jax.experimental.pallas import tpu as pltpu
from jax.sharding import Mesh
from jax.sharding import PartitionSpec as P

MESH = pl.DeviceIdType.MESH
CTX = ("y", "z")
HEAD = ("x", "c")
F32 = jnp.float32
BF16 = jnp.bfloat16
NEG = float("-inf")


def dot_nt(a, b):
    return lax.dot_general(a, b, (((1,), (1,)), ((), ())), preferred_element_type=F32)


def dot_nn(a, b, precision=None):
    return lax.dot_general(
        a, b, (((1,), (0,)), ((), ())), precision=precision, preferred_element_type=F32
    )


def dot_tn(a, b):
    return lax.dot_general(a, b, (((0,), (0,)), ((), ())), preferred_element_type=F32)


def wait_bytes(ref, sem):
    pltpu.make_async_copy(ref, ref, sem).wait()


def kernel(
    q_ref, v_ref, row_ref, book_ref, w_ref, out_ref,
    qin, vin, codes, book, split, vals, qs,
    sums, raw, tot_s, tot_r, pre_s, cache,
    csums, craw, ctot_s, ctot_r, cpre_s, ccache,
    code_sc, fw, aloc, stat, gath, wcol, acc,
    in_sem, z_send, z_recv, y_send, y_recv, w_send, w_recv, w_local, g_send, g_recv, g_other,
    *, ny, nz, nx, nch,
):
    heads, ncodes, width = book_ref.shape
    tokens = q_ref.shape[0] // heads
    sl = ncodes // nz
    part = tokens // nch
    cols = out_ref.shape[1]
    y, z, x, c = (lax.axis_index(name) for name in ("y", "z", "x", "c"))
    scope = jax.named_scope

    def far_first(j):
        step = (j + 1) // 2
        sign = 1 - 2 * lax.rem(j, 2)
        return lax.rem(z + nz // 2 + sign * step + nz, nz)

    def x_at(d):
        return lax.rem(x + d, nx)

    barrier = pltpu.get_barrier_semaphore()

    def greet(j, carry):
        pl.semaphore_signal(barrier, inc=1, device_id={"z": far_first(j)}, device_id_type=MESH)
        return carry

    lax.fori_loop(0, nz - 1, greet, 0)
    for d in range(1, ny):
        there = {"y": lax.rem(y + d, ny)}
        pl.semaphore_signal(barrier, inc=1, device_id=there, device_id_type=MESH)
    peers = [(dx, dc) for dx in range(nx) for dc in range(2)][1:]
    for dx, dc in peers:
        there = {"x": x_at(dx), "c": lax.rem(c + dc, 2)}
        pl.semaphore_signal(barrier, inc=1, device_id=there, device_id_type=MESH)

    loads = []
    for number, (source, target) in enumerate(
        ((row_ref, codes), (v_ref, vin), (book_ref, book), (q_ref, qin))
    ):
        loads.append(pltpu.make_async_copy(source, target, in_sem.at[number]))
        loads[-1].start()

    with scope("load"):
        loads[0].wait()
        loads[1].wait()
    with scope("sums"):
        split[...] = vin[...].astype(F32)
        counts = None
        for h in range(heads):
            vals[h] = split[pl.ds(h, tokens, stride=heads), :].astype(BF16)
            onehot_t = (
                lax.broadcasted_iota(jnp.int32, (ncodes, tokens), 0) == codes[h : h + 1, :]
            ).astype(BF16)
            both = jnp.concatenate([vals[h], jnp.ones((tokens, width), BF16)], axis=1)
            summed = dot_nn(onehot_t, both)
            sums[h] = summed[:, :width].astype(BF16).reshape(nz, sl, width)
            lane = lax.broadcasted_iota(jnp.int32, (ncodes, width), 1)
            code = lax.broadcasted_iota(jnp.int32, (ncodes, width), 0)
            mine = jnp.where(lane == h * sl + lax.rem(code, sl), summed[:, width:], 0.0)
            counted = jnp.sum(mine.reshape(nz, sl, width), axis=1)
            counts = counted if counts is None else counts + counted
        csums[...] = counts.reshape(nz, 1, width)

    def block_scores(h):
        onehot_t = (
            lax.broadcasted_iota(jnp.int32, (ncodes, tokens), 0) == codes[h : h + 1, :]
        ).astype(BF16)
        keys_t = dot_tn(book[h], onehot_t).astype(BF16)
        scale = width ** (-0.5)
        code_sc[h] = dot_nt(qs[h], book[h]) * scale
        scores = dot_nn(qs[h], keys_t) * scale
        rows = lax.broadcasted_iota(jnp.int32, (tokens, tokens), 0)
        ends = lax.broadcasted_iota(jnp.int32, (tokens, tokens), 1)
        scores = jnp.where(rows >= ends, scores, NEG)
        top = jnp.max(scores, axis=1, keepdims=True)
        weights = jnp.exp(scores - top)
        aloc[h] = dot_nn(weights.astype(BF16), vals[h])
        stat[h, 0] = top
        stat[h, 1] = jnp.sum(weights, axis=1, keepdims=True)

    with scope("barrier"):
        pl.semaphore_wait(barrier, nz - 1 + ny - 1 + len(peers))

    def z_push(source, target, chunk):
        def push(j, carry):
            there = far_first(j)
            pltpu.make_async_remote_copy(
                src_ref=source.at[there],
                dst_ref=target.at[z],
                send_sem=z_send.at[chunk],
                recv_sem=z_recv.at[chunk],
                device_id={"z": there},
                device_id_type=MESH,
            ).start()
            return carry

        lax.fori_loop(0, nz - 1, push, 0)
        target[z] = source[z]

    def z_push_band(source, target, chunk, start, count):
        def push(j, carry):
            there = start + lax.rem(z + j, count)

            @pl.when(there != z)
            def _():
                pltpu.make_async_remote_copy(
                    src_ref=source.at[there],
                    dst_ref=target.at[z],
                    send_sem=z_send.at[chunk],
                    recv_sem=z_recv.at[chunk],
                    device_id={"z": there},
                    device_id_type=MESH,
                ).start()

            return carry

        lax.fori_loop(0, count, push, 0)

    with scope("push_raw"):
        z_push(csums, craw, 0)
        for h in range(heads):
            z_push(sums.at[h], raw.at[h], 1 + h)

    def w_slice(dx, dc):
        owner = x_at(dx) * 2 + lax.rem(c + dc, 2)
        return w_ref.at[:, pl.ds(pl.multiple_of(owner * cols, cols), cols)]

    own_w = pltpu.make_async_copy(w_slice(0, 0), wcol.at[0], w_local)
    own_w.start()
    for dx, dc in peers:
        pltpu.make_async_remote_copy(
            src_ref=w_slice(dx, dc),
            dst_ref=wcol.at[(nx - dx) % nx * 2 + dc],
            send_sem=w_send,
            recv_sem=w_recv,
            device_id={"x": x_at(dx), "c": lax.rem(c + dc, 2)},
            device_id_type=MESH,
        ).start()

    with scope("scores"):
        loads[2].wait()
        loads[3].wait()
        split[...] = qin[...].astype(F32)
        for h in range(heads):
            qs[h] = split[pl.ds(h, tokens, stride=heads), :].astype(BF16)
            block_scores(h)

    def y_push(source, target, chunk):
        for d in range(1, ny):
            pltpu.make_async_remote_copy(
                src_ref=source,
                dst_ref=target.at[ny - d],
                send_sem=y_send.at[chunk],
                recv_sem=y_recv.at[chunk],
                device_id={"y": lax.rem(y + d, ny)},
                device_id_type=MESH,
            ).start()

    with scope("wait_craw"):
        wait_bytes(craw.at[pl.ds(0, nz - 1)], z_recv.at[0])
    cbefore, so_far = [], jnp.zeros((1, width), F32)
    for n in range(nz):
        cbefore.append(so_far)
        so_far = so_far + craw[n]
    ctot_s[...] = so_far
    y_push(ctot_s, ctot_r, 0)
    def row_total(h):
        with scope(f"wait_raw{h}"):
            wait_bytes(raw.at[h, pl.ds(0, nz - 1)], z_recv.at[1 + h])
        so_far = raw[h, 0].astype(F32)
        for n in range(1, nz):
            so_far = so_far + raw[h, n].astype(F32)
        tot_s[h] = so_far.astype(BF16)
        y_push(tot_s.at[h], tot_r.at[h], 1 + h)

    def earlier_rows(target):
        total = None
        for d in range(1, ny):
            row = jnp.where(y + d >= ny, target[d].astype(F32), 0.0)
            total = row if total is None else total + row
        return total

    def send_prefix(h):
        with scope(f"wait_y{h}"):
            wait_bytes(tot_r.at[h, pl.ds(1, ny - 1)], y_recv.at[1 + h])
        with scope(f"prefix{h}"):
            so_far = earlier_rows(tot_r.at[h])
            for n in range(nz):
                pre_s[h, n] = so_far.astype(BF16)
                so_far = so_far + raw[h, n].astype(F32)
            cache[h, z] = pre_s[h, z]
            z_push_band(pre_s.at[h], cache.at[h], 4 + h, 0, nz // 4)
            z_push_band(pre_s.at[h], cache.at[h], 4 + h, nz // 4, nz // 4)

    row_total(0)
    with scope("wait_cy"):
        wait_bytes(ctot_r.at[pl.ds(1, ny - 1)], y_recv.at[0])
    above = earlier_rows(ctot_r)
    for n in range(nz):
        cpre_s[n] = cbefore[n] + above
    z_push(cpre_s, ccache, 3)
    for h in range(1, heads):
        row_total(h)
    for h in range(heads):
        send_prefix(h)
    for h in range(heads):
        z_push_band(pre_s.at[h], cache.at[h], 4 + h, nz // 2, nz // 2)

    with scope("wait_ccache"):
        wait_bytes(ccache.at[pl.ds(0, nz - 1)], z_recv.at[3])

    def code_weights(h):
        lane = lax.broadcasted_iota(jnp.int32, (width, ncodes), 0)
        code = lax.broadcasted_iota(jnp.int32, (width, ncodes), 1)
        pick = (lane == h * sl + lax.rem(code, sl)).astype(F32)
        spread = dot_nn(found, pick, lax.Precision.HIGHEST)
        group = lax.broadcasted_iota(jnp.int32, (nz, ncodes), 0)
        where = lax.broadcasted_iota(jnp.int32, (nz, ncodes), 1) // sl
        count = jnp.sum(jnp.where(group == where, spread, 0.0), axis=0, keepdims=True)
        scores = jnp.where(count > 0.0, code_sc[h], NEG)
        top = jnp.maximum(stat[h, 0], jnp.max(scores, axis=1, keepdims=True))
        weights = jnp.exp(scores - top)
        shift = jnp.exp(stat[h, 0] - top)
        den = stat[h, 1] * shift + jnp.sum(weights * count, axis=1, keepdims=True)
        inverse = 1.0 / den
        fw[h] = (weights * inverse).astype(BF16)
        aloc[h] = aloc[h] * (shift * inverse)

    with scope("weights"):
        found = ccache[...].reshape(nz, width)
        for h in range(heads):
            code_weights(h)

    right, left = 1, nx - 1

    def piece(slot, h, r):
        return gath.at[slot[0], slot[1], pl.ds(r * part, part), pl.ds(h * width, width)]

    def arrival(h, r, slot):
        return g_other.at[slot[0]] if slot[1] else g_recv.at[h, slot[0] - 1, r]

    def send(h, r, slot, dx, dc):
        there = ((slot[0] - dx) % nx, (slot[1] + dc) % 2)
        pltpu.make_async_remote_copy(
            src_ref=piece(slot, h, r),
            dst_ref=piece(there, h, r),
            send_sem=g_send.at[1 if dc else 0],
            recv_sem=arrival(h, r, there),
            device_id={"x": x_at(dx), "c": lax.rem(c + dc, 2)},
            device_id_type=MESH,
        ).start()

    def landed(h, r, slot):
        wait_bytes(piece(slot, h, r), arrival(h, r, slot))

    low, high = range(nch // 2), range(nch // 2, nch)
    def finish(h):
        with scope(f"wait_cache{h}"):
            wait_bytes(cache.at[h, pl.ds(0, nz - 1)], z_recv.at[4 + h])
        table = cache[h].reshape(ncodes, width)
        gath[0, 0, :, h * width : (h + 1) * width] = (aloc[h] + dot_nn(fw[h], table)).astype(BF16)
        for r, s in zip((*low, *high), (*high, *low), strict=True):
            send(h, r, (0, 0), right, 0)
            send(h, s, (0, 0), left, 0)
        for r in range(nch):
            send(h, r, (0, 0), 0, 1)

    def relay(h):
        with scope(f"relay{h}"):
            for r, s in zip(low, high, strict=True):
                landed(h, r, (left, 0))
                send(h, r, (left, 0), right, 0)
                send(h, r, (left, 0), 0, 1)
                landed(h, s, (right, 0))
                send(h, s, (right, 0), left, 0)
                send(h, s, (right, 0), 0, 1)
            for r, s in zip(high, low, strict=True):
                landed(h, r, (left, 0))
                send(h, r, (left, 0), 0, 1)
                landed(h, s, (right, 0))
                send(h, s, (right, 0), 0, 1)

    def across(h):
        with scope(f"across{h}"):
            for r, s in zip(low, high, strict=True):
                landed(h, r, (2, 0))
                send(h, r, (2, 0), 0, 1)
                landed(h, s, (2, 0))
                send(h, s, (2, 0), 0, 1)

    def project(slot, first=False):
        add = dot_nn(gath[slot[0], slot[1]], wcol[slot[0] * 2 + slot[1]])
        acc[...] = add if first else acc[...] + add

    finish(0)
    finish(1)
    with scope("wait_w"):
        own_w.wait()
        w_all = wcol.at[pl.ds(1, len(peers))]
        wait_bytes(w_all, w_recv)
        wait_bytes(w_all, w_send)
    project((0, 0), True)
    relay(0)
    relay(1)
    for slot in ((left, 0), (right, 0)):
        project(slot)
    across(0)
    across(1)
    for slot in ((2, 0), (0, 1), (left, 1), (right, 1), (2, 1)):
        if slot[1]:
            with scope("other"):
                wait_bytes(gath.at[slot[0], slot[1]], g_other.at[slot[0]])
        project(slot)
    out_ref[...] = acc[...].astype(BF16)

    with scope("tail"):
        wait_bytes(gath.at[pl.ds(0, 3), 0], g_send.at[0])
        wait_bytes(gath.at[pl.ds(0, nx), 0], g_send.at[1])
        for chunk, ref in ((0, csums), (1, sums.at[0]), (2, sums.at[1])):
            wait_bytes(ref.at[pl.ds(0, nz - 1)], z_send.at[chunk])
        for chunk, ref in ((3, cpre_s), (4, pre_s.at[0]), (5, pre_s.at[1])):
            wait_bytes(ref.at[pl.ds(0, nz - 1)], z_send.at[chunk])
        for chunk, ref in ((0, ctot_r), (1, tot_r.at[0]), (2, tot_r.at[1])):
            wait_bytes(ref.at[pl.ds(1, ny - 1)], y_send.at[chunk])


def on_device(queries, values, codes, codebook, out_weight, *, ny, nz, nx):
    tokens, heads, width = queries.shape
    ncodes = codebook.shape[1]
    sl = ncodes // nz
    cols = out_weight.shape[1] // (nx * 2)
    depth = out_weight.shape[0]
    nch = 4
    anywhere = pl.BlockSpec(memory_space=pl.ANY)
    scratch = [
        pltpu.VMEM((tokens * heads, width), BF16),
        pltpu.VMEM((tokens * heads, width), BF16),
        pltpu.VMEM((heads, tokens), jnp.int32),
        pltpu.VMEM((heads, ncodes, width), BF16),
        pltpu.VMEM((tokens * heads, width), F32),
        pltpu.VMEM((heads, tokens, width), BF16),
        pltpu.VMEM((heads, tokens, width), BF16),
        pltpu.VMEM((heads, nz, sl, width), BF16),
        pltpu.VMEM((heads, nz, sl, width), BF16),
        pltpu.VMEM((heads, sl, width), BF16),
        pltpu.VMEM((heads, ny, sl, width), BF16),
        pltpu.VMEM((heads, nz, sl, width), BF16),
        pltpu.VMEM((heads, nz, sl, width), BF16),
        pltpu.VMEM((nz, 1, width), F32),
        pltpu.VMEM((nz, 1, width), F32),
        pltpu.VMEM((1, width), F32),
        pltpu.VMEM((ny, 1, width), F32),
        pltpu.VMEM((nz, 1, width), F32),
        pltpu.VMEM((nz, 1, width), F32),
        pltpu.VMEM((heads, tokens, ncodes), F32),
        pltpu.VMEM((heads, tokens, ncodes), BF16),
        pltpu.VMEM((heads, tokens, width), F32),
        pltpu.VMEM((heads, 2, tokens, 1), F32),
        pltpu.VMEM((nx, 2, tokens, depth), BF16),
        pltpu.VMEM((nx * 2, depth, cols), BF16),
        pltpu.VMEM((tokens, cols), F32),
        pltpu.SemaphoreType.DMA((4,)),
        pltpu.SemaphoreType.DMA((6,)),
        pltpu.SemaphoreType.DMA((6,)),
        pltpu.SemaphoreType.DMA((3,)),
        pltpu.SemaphoreType.DMA((3,)),
        pltpu.SemaphoreType.DMA,
        pltpu.SemaphoreType.DMA,
        pltpu.SemaphoreType.DMA,
        pltpu.SemaphoreType.DMA((2,)),
        pltpu.SemaphoreType.DMA((heads, nx - 1, nch)),
        pltpu.SemaphoreType.DMA((nx,)),
    ]
    return pl.pallas_call(
        functools.partial(kernel, ny=ny, nz=nz, nx=nx, nch=nch),
        out_shape=pltpu.VMEM((tokens, cols), BF16),
        in_specs=[anywhere] * 5,
        out_specs=pl.BlockSpec(memory_space=pltpu.VMEM),
        scratch_shapes=scratch,
        compiler_params=pltpu.CompilerParams(collective_id=0, has_side_effects=True),
        name="vq_layer",
    )(
        queries.reshape(tokens * heads, width),
        values.reshape(tokens * heads, width),
        codes.T,
        codebook,
        out_weight,
    )


def layer(mesh, ny, nz, nx):
    finer = Mesh(mesh.devices.reshape(ny, nz, nx, 2), ("y", "z", "x", "c"))
    placed = (
        P(CTX, HEAD, None),
        P(CTX, HEAD, None),
        P(CTX, HEAD),
        P(HEAD, None, None),
        P(HEAD, None),
    )
    return jax.shard_map(
        functools.partial(on_device, ny=ny, nz=nz, nx=nx),
        mesh=finer,
        in_specs=placed,
        out_specs=P(CTX, HEAD),
        check_vma=False,
    )


def solution(mesh):
    return layer(mesh, 4, 16, 4)
```

```python
import functools

import jax
import jax.numpy as jnp
from jax import lax
from jax.experimental import pallas as pl
from jax.experimental.pallas import tpu as pltpu
from jax.sharding import Mesh
from jax.sharding import PartitionSpec as P

MESH = pl.DeviceIdType.MESH
CTX = ("y", "z")
HEAD = ("x", "c")
F32 = jnp.float32
BF16 = jnp.bfloat16
NEG = float("-inf")


def dot_nt(a, b):
    return lax.dot_general(a, b, (((1,), (1,)), ((), ())), preferred_element_type=F32)


def dot_nn(a, b, precision=None):
    return lax.dot_general(
        a, b, (((1,), (0,)), ((), ())), precision=precision, preferred_element_type=F32
    )


def dot_tn(a, b):
    return lax.dot_general(a, b, (((0,), (0,)), ((), ())), preferred_element_type=F32)


def wait_bytes(ref, sem):
    pltpu.make_async_copy(ref, ref, sem).wait()


def kernel(
    q_ref, v_ref, row_ref, book_ref, w_ref, out_ref,
    qin, vin, codes, book, split, vals, qs,
    sums, theirs, gsum, raw, tot_s, tot_r, pre_s, cache,
    csums, craw, ctot_s, ctot_r, cpre_s, ccache,
    code_sc, fw, aloc, stat, gath, wcol, acc,
    in_sem, z_send, z_recv, y_send, y_recv, w_send, w_recv, w_local, g_send, g_recv, g_other,
    *, ny, nz, nx, nch,
):
    heads, ncodes, width = book_ref.shape
    tokens = q_ref.shape[0] // heads
    sl = ncodes // nz
    part = tokens // nch
    cols = out_ref.shape[1]
    y, z, x, c = (lax.axis_index(name) for name in ("y", "z", "x", "c"))
    scope = jax.named_scope

    def far_first(j):
        step = (j + 1) // 2
        sign = 1 - 2 * lax.rem(j, 2)
        return lax.rem(z + nz // 2 + sign * step + nz, nz)

    def x_at(d):
        return lax.rem(x + d, nx)

    npair = nz // 2
    odd, pair = lax.rem(z, 2), z // 2
    partner = z + 1 - 2 * odd

    def slice_of(at):
        return lax.rem(at, 2) * npair + at // 2

    def far_pair(j):
        step = (j + 1) // 2
        sign = 1 - 2 * lax.rem(j, 2)
        return lax.rem(pair + npair // 2 + sign * step + npair, npair)

    barrier = pltpu.get_barrier_semaphore()

    def greet(j, carry):
        pl.semaphore_signal(barrier, inc=1, device_id={"z": far_first(j)}, device_id_type=MESH)
        return carry

    lax.fori_loop(0, nz - 1, greet, 0)
    for d in range(1, ny):
        there = {"y": lax.rem(y + d, ny)}
        pl.semaphore_signal(barrier, inc=1, device_id=there, device_id_type=MESH)
    peers = [(dx, dc) for dx in range(nx) for dc in range(2)][1:]
    for dx, dc in peers:
        there = {"x": x_at(dx), "c": lax.rem(c + dc, 2)}
        pl.semaphore_signal(barrier, inc=1, device_id=there, device_id_type=MESH)

    loads = []
    for number, (source, target) in enumerate(
        ((row_ref, codes), (v_ref, vin), (book_ref, book), (q_ref, qin))
    ):
        loads.append(pltpu.make_async_copy(source, target, in_sem.at[number]))
        loads[-1].start()

    with scope("load"):
        loads[0].wait()
        loads[1].wait()
    with scope("sums"):
        split[...] = vin[...].astype(F32)
        counts = None
        for h in range(heads):
            vals[h] = split[pl.ds(h, tokens, stride=heads), :].astype(BF16)
            onehot_t = (
                lax.broadcasted_iota(jnp.int32, (ncodes, tokens), 0) == codes[h : h + 1, :]
            ).astype(BF16)
            both = jnp.concatenate([vals[h], jnp.ones((tokens, width), BF16)], axis=1)
            summed = dot_nn(onehot_t, both)
            sums[h] = summed[:, :width].astype(BF16).reshape(nz, sl, width)
            lane = lax.broadcasted_iota(jnp.int32, (ncodes, width), 1)
            code = lax.broadcasted_iota(jnp.int32, (ncodes, width), 0)
            mine = jnp.where(lane == h * sl + lax.rem(code, sl), summed[:, width:], 0.0)
            counted = jnp.sum(mine.reshape(nz, sl, width), axis=1)
            counts = counted if counts is None else counts + counted
        csums[...] = counts.reshape(nz, 1, width)

    def block_scores(h):
        onehot_t = (
            lax.broadcasted_iota(jnp.int32, (ncodes, tokens), 0) == codes[h : h + 1, :]
        ).astype(BF16)
        keys_t = dot_tn(book[h], onehot_t).astype(BF16)
        scale = width ** (-0.5)
        code_sc[h] = dot_nt(qs[h], book[h]) * scale
        scores = dot_nn(qs[h], keys_t) * scale
        rows = lax.broadcasted_iota(jnp.int32, (tokens, tokens), 0)
        ends = lax.broadcasted_iota(jnp.int32, (tokens, tokens), 1)
        scores = jnp.where(rows >= ends, scores, NEG)
        top = jnp.max(scores, axis=1, keepdims=True)
        weights = jnp.exp(scores - top)
        aloc[h] = dot_nn(weights.astype(BF16), vals[h])
        stat[h, 0] = top
        stat[h, 1] = jnp.sum(weights, axis=1, keepdims=True)

    with scope("barrier"):
        pl.semaphore_wait(barrier, nz - 1 + ny - 1 + len(peers))

    def z_copy(source, target, chunk, there):
        return pltpu.make_async_remote_copy(
            src_ref=source,
            dst_ref=target,
            send_sem=z_send.at[chunk],
            recv_sem=z_recv.at[chunk],
            device_id={"z": there},
            device_id_type=MESH,
        )

    def push_counts():
        def push(j, carry):
            there = far_first(j)
            z_copy(csums.at[slice_of(there)], craw.at[z], 0, there).start()
            return carry

        lax.fori_loop(0, nz - 1, push, 0)
        craw[z] = csums[slice_of(z)]

    def push_counts_back():
        def push(j, carry):
            there = far_first(j)
            z_copy(cpre_s.at[there], ccache.at[slice_of(z)], 3, there).start()
            return carry

        lax.fori_loop(0, nz - 1, push, 0)
        ccache[slice_of(z)] = cpre_s[z]

    def push_pair_sums(h):
        def push(j, carry):
            there = far_pair(j)
            z_copy(gsum.at[h, there], raw.at[h, pair], 1 + h, 2 * there + odd).start()
            return carry

        lax.fori_loop(0, npair - 1, push, 0)
        raw[h, pair] = gsum[h, pair]

    def z_push_band(h, start, count):
        def push(j, carry):
            there = start + lax.rem(z + j, count)

            @pl.when(there != z)
            def _():
                z_copy(pre_s.at[h, there // 2], cache.at[h, slice_of(z)], 4 + h, there).start()

            return carry

        lax.fori_loop(0, count, push, 0)

    def half_rows(ref, h, which):
        return ref.at[h, pl.ds(which * npair, npair)]

    def swap(h):
        return z_copy(half_rows(sums, h, 1 - odd), half_rows(theirs, h, 1 - odd), 6 + h, partner)

    def fill(h):
        return z_copy(half_rows(sums, h, 0), half_rows(theirs, h, 0), 8 + h, partner)

    with scope("push_raw"):
        push_counts()
        for h in range(heads):
            swap(h).start()

    def w_slice(dx, dc):
        owner = x_at(dx) * 2 + lax.rem(c + dc, 2)
        return w_ref.at[:, pl.ds(pl.multiple_of(owner * cols, cols), cols)]

    own_w = pltpu.make_async_copy(w_slice(0, 0), wcol.at[0], w_local)
    own_w.start()
    for dx, dc in peers:
        pltpu.make_async_remote_copy(
            src_ref=w_slice(dx, dc),
            dst_ref=wcol.at[(nx - dx) % nx * 2 + dc],
            send_sem=w_send,
            recv_sem=w_recv,
            device_id={"x": x_at(dx), "c": lax.rem(c + dc, 2)},
            device_id_type=MESH,
        ).start()

    with scope("scores"):
        loads[2].wait()
        loads[3].wait()
        split[...] = qin[...].astype(F32)
        for h in range(heads):
            qs[h] = split[pl.ds(h, tokens, stride=heads), :].astype(BF16)
            block_scores(h)

    for h in range(heads):
        with scope(f"wait_swap{h}"):
            wait_bytes(half_rows(theirs, h, odd), z_recv.at[6 + h])
        own = half_rows(sums, h, odd)[...].astype(F32)
        gsum[h] = (own + half_rows(theirs, h, odd)[...].astype(F32)).astype(BF16)
        push_pair_sums(h)

    @pl.when(odd == 0)
    def _():
        for h in range(heads):
            fill(h).start()

    def y_copy(source, target, chunk, d):
        return pltpu.make_async_remote_copy(
            src_ref=source,
            dst_ref=target.at[d],
            send_sem=y_send.at[chunk, d - 1],
            recv_sem=y_recv.at[chunk, d - 1],
            device_id={"y": lax.rem(y + d, ny)},
            device_id_type=MESH,
        )

    def y_push(source, target, chunk):
        for d in range(1, ny):

            @pl.when(y + d < ny)
            def _(d=d):
                y_copy(source, target, chunk, d).start()

    with scope("wait_craw"):
        wait_bytes(craw.at[pl.ds(0, nz - 1)], z_recv.at[0])
    cbefore, so_far = [], jnp.zeros((1, width), F32)
    for n in range(nz):
        cbefore.append(so_far)
        so_far = so_far + craw[n]
    ctot_s[...] = so_far
    y_push(ctot_s, ctot_r, 0)
    def row_total(h):
        with scope(f"wait_raw{h}"):
            wait_bytes(raw.at[h, pl.ds(0, npair - 1)], z_recv.at[1 + h])
        so_far = raw[h, 0].astype(F32)
        for n in range(1, npair):
            so_far = so_far + raw[h, n].astype(F32)
        tot_s[h] = so_far.astype(BF16)
        y_push(tot_s.at[h], tot_r.at[h], 1 + h)

    def earlier_rows(source, target, chunk):
        total = None
        for d in range(1, ny):

            @pl.when(y >= d)
            def _(d=d):
                y_copy(source, target, chunk, d).wait_recv()

            row = jnp.where(y >= d, target[d].astype(F32), 0.0)
            total = row if total is None else total + row
        return total

    def send_prefix(h):
        with scope(f"wait_y{h}"):
            so_far = earlier_rows(tot_s.at[h], tot_r.at[h], 1 + h)
        with scope(f"prefix{h}"):
            for n in range(npair):
                pre_s[h, n] = so_far.astype(BF16)
                so_far = so_far + raw[h, n].astype(F32)
            cache[h, slice_of(z)] = pre_s[h, pair]
            z_push_band(h, 0, nz // 4)
            z_push_band(h, nz // 4, nz // 4)

    row_total(0)
    with scope("wait_cy"):
        above = earlier_rows(ctot_s, ctot_r, 0)
    for n in range(nz):
        cpre_s[n] = cbefore[n] + above
    push_counts_back()
    for h in range(1, heads):
        row_total(h)
    for h in range(heads):
        send_prefix(h)
    for h in range(heads):
        z_push_band(h, nz // 2, nz // 2)

    with scope("wait_ccache"):
        wait_bytes(ccache.at[pl.ds(0, nz - 1)], z_recv.at[3])

    def code_weights(h):
        lane = lax.broadcasted_iota(jnp.int32, (width, ncodes), 0)
        code = lax.broadcasted_iota(jnp.int32, (width, ncodes), 1)
        pick = (lane == h * sl + lax.rem(code, sl)).astype(F32)
        spread = dot_nn(found, pick, lax.Precision.HIGHEST)
        group = lax.broadcasted_iota(jnp.int32, (nz, ncodes), 0)
        where = lax.broadcasted_iota(jnp.int32, (nz, ncodes), 1) // sl
        count = jnp.sum(jnp.where(group == where, spread, 0.0), axis=0, keepdims=True)
        scores = jnp.where(count > 0.0, code_sc[h], NEG)
        top = jnp.maximum(stat[h, 0], jnp.max(scores, axis=1, keepdims=True))
        weights = jnp.exp(scores - top)
        shift = jnp.exp(stat[h, 0] - top)
        den = stat[h, 1] * shift + jnp.sum(weights * count, axis=1, keepdims=True)
        inverse = 1.0 / den
        fw[h] = (weights * inverse).astype(BF16)
        aloc[h] = aloc[h] * (shift * inverse)

    with scope("weights"):
        found = ccache[...].reshape(nz, width)
        for h in range(heads):
            code_weights(h)

    right, left = 1, nx - 1

    def piece(slot, h, r):
        return gath.at[slot[0], slot[1], h, pl.ds(r * part, part)]

    def arrival(h, r, slot):
        return g_other.at[slot[0]] if slot[1] else g_recv.at[h, slot[0] - 1, r]

    def send(h, r, slot, dx, dc):
        there = ((slot[0] - dx) % nx, (slot[1] + dc) % 2)
        pltpu.make_async_remote_copy(
            src_ref=piece(slot, h, r),
            dst_ref=piece(there, h, r),
            send_sem=g_send.at[1 if dc else 0],
            recv_sem=arrival(h, r, there),
            device_id={"x": x_at(dx), "c": lax.rem(c + dc, 2)},
            device_id_type=MESH,
        ).start()

    def landed(h, r, slot):
        wait_bytes(piece(slot, h, r), arrival(h, r, slot))

    low, high = range(nch // 2), range(nch // 2, nch)
    def finish(h):
        with scope(f"wait_cache{h}"):
            wait_bytes(cache.at[h, pl.ds(0, nz - 1)], z_recv.at[4 + h])

        @pl.when(odd == 1)
        def _():
            fill(h).wait_recv()

        mine = jnp.where(odd == 1, theirs[h].astype(F32), 0.0)
        table = (cache[h].astype(F32) + mine).astype(BF16).reshape(ncodes, width)
        gath[0, 0, h] = (aloc[h] + dot_nn(fw[h], table)).astype(BF16)
        for r, s in zip((*low, *high), (*high, *low), strict=True):
            send(h, r, (0, 0), right, 0)
            send(h, s, (0, 0), left, 0)
        for r in range(nch):
            send(h, r, (0, 0), 0, 1)

    def relay(h):
        with scope(f"relay{h}"):
            for r, s in zip(low, high, strict=True):
                landed(h, r, (left, 0))
                send(h, r, (left, 0), right, 0)
                send(h, r, (left, 0), 0, 1)
                landed(h, s, (right, 0))
                send(h, s, (right, 0), left, 0)
                send(h, s, (right, 0), 0, 1)
            for r, s in zip(high, low, strict=True):
                landed(h, r, (left, 0))
                send(h, r, (left, 0), 0, 1)
                landed(h, s, (right, 0))
                send(h, s, (right, 0), 0, 1)

    def across(h):
        with scope(f"across{h}"):
            for r, s in zip(low, high, strict=True):
                landed(h, r, (2, 0))
                send(h, r, (2, 0), 0, 1)
                landed(h, s, (2, 0))
                send(h, s, (2, 0), 0, 1)

    def project(slot, first=False):
        rows = jnp.concatenate([gath[slot[0], slot[1], h] for h in range(heads)], axis=1)
        add = dot_nn(rows, wcol[slot[0] * 2 + slot[1]])
        acc[...] = add if first else acc[...] + add

    finish(0)
    finish(1)
    with scope("wait_w"):
        own_w.wait()
        w_all = wcol.at[pl.ds(1, len(peers))]
        wait_bytes(w_all, w_recv)
        wait_bytes(w_all, w_send)
    project((0, 0), True)
    relay(0)
    relay(1)
    for slot in ((left, 0), (right, 0)):
        project(slot)
    across(0)
    across(1)
    for slot in ((2, 0), (0, 1), (left, 1), (right, 1), (2, 1)):
        if slot[1]:
            with scope("other"):
                wait_bytes(gath.at[slot[0], slot[1]], g_other.at[slot[0]])
        project(slot)
    out_ref[...] = acc[...].astype(BF16)

    with scope("tail"):
        wait_bytes(gath.at[pl.ds(0, 3), 0], g_send.at[0])
        wait_bytes(gath.at[pl.ds(0, nx), 0], g_send.at[1])
        for chunk, ref in ((0, csums), (3, csums), (4, cache.at[0]), (5, cache.at[1])):
            wait_bytes(ref.at[pl.ds(0, nz - 1)], z_send.at[chunk])
        for h in range(heads):
            wait_bytes(raw.at[h, pl.ds(0, npair - 1)], z_send.at[1 + h])
            swap(h).wait_send()

        @pl.when(odd == 0)
        def _():
            for h in range(heads):
                fill(h).wait_send()

        for chunk, source, target in (
            (0, ctot_s, ctot_r),
            (1, tot_s.at[0], tot_r.at[0]),
            (2, tot_s.at[1], tot_r.at[1]),
        ):
            for d in range(1, ny):

                @pl.when(y + d < ny)
                def _(chunk=chunk, source=source, target=target, d=d):
                    y_copy(source, target, chunk, d).wait_send()


def on_device(queries, values, codes, codebook, out_weight, *, ny, nz, nx):
    tokens, heads, width = queries.shape
    ncodes = codebook.shape[1]
    sl = ncodes // nz
    cols = out_weight.shape[1] // (nx * 2)
    depth = out_weight.shape[0]
    nch = 4
    anywhere = pl.BlockSpec(memory_space=pl.ANY)
    scratch = [
        pltpu.VMEM((tokens * heads, width), BF16),
        pltpu.VMEM((tokens * heads, width), BF16),
        pltpu.VMEM((heads, tokens), jnp.int32),
        pltpu.VMEM((heads, ncodes, width), BF16),
        pltpu.VMEM((tokens * heads, width), F32),
        pltpu.VMEM((heads, tokens, width), BF16),
        pltpu.VMEM((heads, tokens, width), BF16),
        pltpu.VMEM((heads, nz, sl, width), BF16),
        pltpu.VMEM((heads, nz, sl, width), BF16),
        pltpu.VMEM((heads, nz // 2, sl, width), BF16),
        pltpu.VMEM((heads, nz // 2, sl, width), BF16),
        pltpu.VMEM((heads, sl, width), BF16),
        pltpu.VMEM((heads, ny, sl, width), BF16),
        pltpu.VMEM((heads, nz // 2, sl, width), BF16),
        pltpu.VMEM((heads, nz, sl, width), BF16),
        pltpu.VMEM((nz, 1, width), F32),
        pltpu.VMEM((nz, 1, width), F32),
        pltpu.VMEM((1, width), F32),
        pltpu.VMEM((ny, 1, width), F32),
        pltpu.VMEM((nz, 1, width), F32),
        pltpu.VMEM((nz, 1, width), F32),
        pltpu.VMEM((heads, tokens, ncodes), F32),
        pltpu.VMEM((heads, tokens, ncodes), BF16),
        pltpu.VMEM((heads, tokens, width), F32),
        pltpu.VMEM((heads, 2, tokens, 1), F32),
        pltpu.VMEM((nx, 2, heads, tokens, width), BF16),
        pltpu.VMEM((nx * 2, depth, cols), BF16),
        pltpu.VMEM((tokens, cols), F32),
        pltpu.SemaphoreType.DMA((4,)),
        pltpu.SemaphoreType.DMA((10,)),
        pltpu.SemaphoreType.DMA((10,)),
        pltpu.SemaphoreType.DMA((3, ny - 1)),
        pltpu.SemaphoreType.DMA((3, ny - 1)),
        pltpu.SemaphoreType.DMA,
        pltpu.SemaphoreType.DMA,
        pltpu.SemaphoreType.DMA,
        pltpu.SemaphoreType.DMA((2,)),
        pltpu.SemaphoreType.DMA((heads, nx - 1, nch)),
        pltpu.SemaphoreType.DMA((nx,)),
    ]
    return pl.pallas_call(
        functools.partial(kernel, ny=ny, nz=nz, nx=nx, nch=nch),
        out_shape=pltpu.VMEM((tokens, cols), BF16),
        in_specs=[anywhere] * 5,
        out_specs=pl.BlockSpec(memory_space=pltpu.VMEM),
        scratch_shapes=scratch,
        compiler_params=pltpu.CompilerParams(collective_id=0, has_side_effects=True),
        name="vq_layer",
    )(
        queries.reshape(tokens * heads, width),
        values.reshape(tokens * heads, width),
        codes.T,
        codebook,
        out_weight,
    )


def layer(mesh, ny, nz, nx):
    finer = Mesh(mesh.devices.reshape(ny, nz, nx, 2), ("y", "z", "x", "c"))
    placed = (
        P(CTX, HEAD, None),
        P(CTX, HEAD, None),
        P(CTX, HEAD),
        P(HEAD, None, None),
        P(HEAD, None),
    )
    return jax.shard_map(
        functools.partial(on_device, ny=ny, nz=nz, nx=nx),
        mesh=finer,
        in_specs=placed,
        out_specs=P(CTX, HEAD),
        check_vma=False,
    )


def solution(mesh):
    return layer(mesh, 4, 16, 4)
```

```python
import functools

import jax
import jax.numpy as jnp
from jax import lax
from jax.experimental import pallas as pl
from jax.experimental.pallas import tpu as pltpu
from jax.sharding import Mesh
from jax.sharding import PartitionSpec as P

MESH = pl.DeviceIdType.MESH
CTX = ("y", "z")
HEAD = ("x", "c")
F32 = jnp.float32
BF16 = jnp.bfloat16
NEG = float("-inf")


def dot_nt(a, b):
    return lax.dot_general(a, b, (((1,), (1,)), ((), ())), preferred_element_type=F32)


def dot_nn(a, b, precision=None):
    return lax.dot_general(
        a, b, (((1,), (0,)), ((), ())), precision=precision, preferred_element_type=F32
    )


def dot_tn(a, b):
    return lax.dot_general(a, b, (((0,), (0,)), ((), ())), preferred_element_type=F32)


def wait_bytes(ref, sem):
    pltpu.make_async_copy(ref, ref, sem).wait()


def kernel(
    q_ref, v_ref, row_ref, book_ref, w_ref, out_ref,
    qin, vin, codes, book, split, vals, qs,
    sums, theirs, gsum, raw, tot_s, tot_r, pre_s, cache,
    csums, craw, ctot_s, ctot_r, cpre_s, ccache,
    code_sc, fw, aloc, stat, gath, wcol, acc,
    in_sem, z_send, z_recv, y_send, y_recv, w_send, w_recv, w_local, g_send, g_recv, g_slot,
    *, ny, nz, nx, nch,
):
    heads, ncodes, width = book_ref.shape
    tokens = q_ref.shape[0] // heads
    sl = ncodes // nz
    part = tokens // nch
    cols = out_ref.shape[1]
    y, z, x, c = (lax.axis_index(name) for name in ("y", "z", "x", "c"))
    scope = jax.named_scope

    def far_first(j):
        step = (j + 1) // 2
        sign = 1 - 2 * lax.rem(j, 2)
        return lax.rem(z + nz // 2 + sign * step + nz, nz)

    def x_at(d):
        return lax.rem(x + d, nx)

    npair = nz // 2
    odd, pair = lax.rem(z, 2), z // 2
    partner = z + 1 - 2 * odd

    def slice_of(at):
        return lax.rem(at, 2) * npair + at // 2

    def far_pair(j):
        step = (j + 1) // 2
        sign = 1 - 2 * lax.rem(j, 2)
        return lax.rem(pair + npair // 2 + sign * step + npair, npair)

    barrier = pltpu.get_barrier_semaphore()

    def greet(j, carry):
        pl.semaphore_signal(barrier, inc=1, device_id={"z": far_first(j)}, device_id_type=MESH)
        return carry

    lax.fori_loop(0, nz - 1, greet, 0)
    for d in range(1, ny):
        there = {"y": lax.rem(y + d, ny)}
        pl.semaphore_signal(barrier, inc=1, device_id=there, device_id_type=MESH)
    peers = [(dx, dc) for dx in range(nx) for dc in range(2)][1:]
    for dx, dc in peers:
        there = {"x": x_at(dx), "c": lax.rem(c + dc, 2)}
        pl.semaphore_signal(barrier, inc=1, device_id=there, device_id_type=MESH)

    loads = []
    for number, (source, target) in enumerate(
        ((row_ref, codes), (v_ref, vin), (book_ref, book), (q_ref, qin))
    ):
        loads.append(pltpu.make_async_copy(source, target, in_sem.at[number]))
        loads[-1].start()

    with scope("load"):
        loads[0].wait()
        loads[1].wait()
    with scope("sums"):
        split[...] = vin[...].astype(F32)
        counts = None
        for h in range(heads):
            vals[h] = split[pl.ds(h, tokens, stride=heads), :].astype(BF16)
            onehot_t = (
                lax.broadcasted_iota(jnp.int32, (ncodes, tokens), 0) == codes[h : h + 1, :]
            ).astype(BF16)
            both = jnp.concatenate([vals[h], jnp.ones((tokens, width), BF16)], axis=1)
            summed = dot_nn(onehot_t, both)
            sums[h] = summed[:, :width].astype(BF16).reshape(nz, sl, width)
            lane = lax.broadcasted_iota(jnp.int32, (ncodes, width), 1)
            code = lax.broadcasted_iota(jnp.int32, (ncodes, width), 0)
            mine = jnp.where(lane == h * sl + lax.rem(code, sl), summed[:, width:], 0.0)
            counted = jnp.sum(mine.reshape(nz, sl, width), axis=1)
            counts = counted if counts is None else counts + counted
        csums[...] = counts.reshape(nz, 1, width)

    def block_scores(h):
        onehot_t = (
            lax.broadcasted_iota(jnp.int32, (ncodes, tokens), 0) == codes[h : h + 1, :]
        ).astype(BF16)
        keys_t = dot_tn(book[h], onehot_t).astype(BF16)
        scale = width ** (-0.5)
        code_sc[h] = dot_nt(qs[h], book[h]) * scale
        scores = dot_nn(qs[h], keys_t) * scale
        rows = lax.broadcasted_iota(jnp.int32, (tokens, tokens), 0)
        ends = lax.broadcasted_iota(jnp.int32, (tokens, tokens), 1)
        scores = jnp.where(rows >= ends, scores, NEG)
        top = jnp.max(scores, axis=1, keepdims=True)
        weights = jnp.exp(scores - top)
        aloc[h] = dot_nn(weights.astype(BF16), vals[h])
        stat[h, 0] = top
        stat[h, 1] = jnp.sum(weights, axis=1, keepdims=True)

    with scope("barrier"):
        pl.semaphore_wait(barrier, nz - 1 + ny - 1 + len(peers))

    def z_copy(source, target, chunk, there):
        return pltpu.make_async_remote_copy(
            src_ref=source,
            dst_ref=target,
            send_sem=z_send.at[chunk],
            recv_sem=z_recv.at[chunk],
            device_id={"z": there},
            device_id_type=MESH,
        )

    def push_counts():
        def push(j, carry):
            there = far_first(j)
            z_copy(csums.at[slice_of(there)], craw.at[z], 0, there).start()
            return carry

        lax.fori_loop(0, nz - 1, push, 0)
        craw[z] = csums[slice_of(z)]

    def push_counts_back():
        def push(j, carry):
            there = far_first(j)
            z_copy(cpre_s.at[there], ccache.at[slice_of(z)], 3, there).start()
            return carry

        lax.fori_loop(0, nz - 1, push, 0)
        ccache[slice_of(z)] = cpre_s[z]

    def push_pair_sums(h):
        def push(j, carry):
            there = far_pair(j)
            z_copy(gsum.at[h, there], raw.at[h, pair], 1 + h, 2 * there + odd).start()
            return carry

        lax.fori_loop(0, npair - 1, push, 0)
        raw[h, pair] = gsum[h, pair]

    def z_push_band(h, start, count):
        def push(j, carry):
            there = start + lax.rem(z + j, count)

            @pl.when(there != z)
            def _():
                z_copy(pre_s.at[h, there // 2], cache.at[h, slice_of(z)], 4 + h, there).start()

            return carry

        lax.fori_loop(0, count, push, 0)

    def half_rows(ref, h, which):
        return ref.at[h, pl.ds(which * npair, npair)]

    def swap(h):
        return z_copy(half_rows(sums, h, 1 - odd), half_rows(theirs, h, 1 - odd), 6 + h, partner)

    def fill(h):
        return z_copy(half_rows(sums, h, 0), half_rows(theirs, h, 0), 8 + h, partner)

    with scope("push_raw"):
        push_counts()
        for h in range(heads):
            swap(h).start()

    def w_slice(dx, dc):
        owner = x_at(dx) * 2 + lax.rem(c + dc, 2)
        return w_ref.at[:, pl.ds(pl.multiple_of(owner * cols, cols), cols)]

    own_w = pltpu.make_async_copy(w_slice(0, 0), wcol.at[0], w_local)
    own_w.start()
    for dx, dc in peers:
        pltpu.make_async_remote_copy(
            src_ref=w_slice(dx, dc),
            dst_ref=wcol.at[(nx - dx) % nx * 2 + dc],
            send_sem=w_send,
            recv_sem=w_recv,
            device_id={"x": x_at(dx), "c": lax.rem(c + dc, 2)},
            device_id_type=MESH,
        ).start()

    with scope("scores"):
        loads[2].wait()
        loads[3].wait()
        split[...] = qin[...].astype(F32)
        for h in range(heads):
            qs[h] = split[pl.ds(h, tokens, stride=heads), :].astype(BF16)
            block_scores(h)

    for h in range(heads):
        with scope(f"wait_swap{h}"):
            wait_bytes(half_rows(theirs, h, odd), z_recv.at[6 + h])
        own = half_rows(sums, h, odd)[...].astype(F32)
        gsum[h] = (own + half_rows(theirs, h, odd)[...].astype(F32)).astype(BF16)
        push_pair_sums(h)

    @pl.when(odd == 0)
    def _():
        for h in range(heads):
            fill(h).start()

    def y_copy(source, target, chunk, d):
        return pltpu.make_async_remote_copy(
            src_ref=source,
            dst_ref=target.at[d],
            send_sem=y_send.at[chunk, d - 1],
            recv_sem=y_recv.at[chunk, d - 1],
            device_id={"y": lax.rem(y + d, ny)},
            device_id_type=MESH,
        )

    def y_push(source, target, chunk):
        for d in range(1, ny):

            @pl.when(y + d < ny)
            def _(d=d):
                y_copy(source, target, chunk, d).start()

    with scope("wait_craw"):
        wait_bytes(craw.at[pl.ds(0, nz - 1)], z_recv.at[0])
    cbefore, so_far = [], jnp.zeros((1, width), F32)
    for n in range(nz):
        cbefore.append(so_far)
        so_far = so_far + craw[n]
    ctot_s[...] = so_far
    y_push(ctot_s, ctot_r, 0)
    def row_total(h):
        with scope(f"wait_raw{h}"):
            wait_bytes(raw.at[h, pl.ds(0, npair - 1)], z_recv.at[1 + h])
        so_far = raw[h, 0].astype(F32)
        for n in range(1, npair):
            so_far = so_far + raw[h, n].astype(F32)
        tot_s[h] = so_far.astype(BF16)
        y_push(tot_s.at[h], tot_r.at[h], 1 + h)

    def earlier_rows(source, target, chunk):
        total = None
        for d in range(1, ny):

            @pl.when(y >= d)
            def _(d=d):
                y_copy(source, target, chunk, d).wait_recv()

            row = jnp.where(y >= d, target[d].astype(F32), 0.0)
            total = row if total is None else total + row
        return total

    def send_prefix(h):
        with scope(f"wait_y{h}"):
            so_far = earlier_rows(tot_s.at[h], tot_r.at[h], 1 + h)
        with scope(f"prefix{h}"):
            for n in range(npair):
                pre_s[h, n] = so_far.astype(BF16)
                so_far = so_far + raw[h, n].astype(F32)
            cache[h, slice_of(z)] = pre_s[h, pair]
            z_push_band(h, 0, nz // 4)
            z_push_band(h, nz // 4, nz // 4)

    row_total(0)
    with scope("wait_cy"):
        above = earlier_rows(ctot_s, ctot_r, 0)
    for n in range(nz):
        cpre_s[n] = cbefore[n] + above
    push_counts_back()
    for h in range(1, heads):
        row_total(h)
    for h in range(heads):
        send_prefix(h)
    for h in range(heads):
        z_push_band(h, nz // 2, nz // 2)

    with scope("wait_ccache"):
        wait_bytes(ccache.at[pl.ds(0, nz - 1)], z_recv.at[3])

    def code_weights(h):
        lane = lax.broadcasted_iota(jnp.int32, (width, ncodes), 0)
        code = lax.broadcasted_iota(jnp.int32, (width, ncodes), 1)
        pick = (lane == h * sl + lax.rem(code, sl)).astype(F32)
        spread = dot_nn(found, pick, lax.Precision.HIGHEST)
        group = lax.broadcasted_iota(jnp.int32, (nz, ncodes), 0)
        where = lax.broadcasted_iota(jnp.int32, (nz, ncodes), 1) // sl
        count = jnp.sum(jnp.where(group == where, spread, 0.0), axis=0, keepdims=True)
        scores = jnp.where(count > 0.0, code_sc[h], NEG)
        top = jnp.maximum(stat[h, 0], jnp.max(scores, axis=1, keepdims=True))
        weights = jnp.exp(scores - top)
        shift = jnp.exp(stat[h, 0] - top)
        den = stat[h, 1] * shift + jnp.sum(weights * count, axis=1, keepdims=True)
        inverse = 1.0 / den
        fw[h] = (weights * inverse).astype(BF16)
        aloc[h] = aloc[h] * (shift * inverse)

    with scope("weights"):
        found = ccache[...].reshape(nz, width)
        for h in range(heads):
            code_weights(h)

    right, left, beyond = 1, nx - 1, 2
    low, high = range(nch // 2), range(nch // 2, nch)

    def piece(slot, h, r):
        return gath.at[slot[0] * 2 + slot[1], h, pl.ds(r * part, part)]

    def send(h, r, slot, dx, dc, whole=False):
        there = ((slot[0] - dx) % nx, (slot[1] + dc) % 2)
        number = there[0] * 2 + there[1]
        pltpu.make_async_remote_copy(
            src_ref=piece(slot, h, r),
            dst_ref=piece(there, h, r),
            send_sem=g_send.at[0 if dx else 1],
            recv_sem=g_slot.at[number] if whole else g_recv.at[number - 2, h, r],
            device_id={"x": x_at(dx), "c": lax.rem(c + dc, 2)},
            device_id_type=MESH,
        ).start()

    def landed(h, r, slot):
        wait_bytes(piece(slot, h, r), g_recv.at[slot[0] * 2 + slot[1] - 2, h, r])

    def landed_whole(slot):
        number = slot[0] * 2 + slot[1]
        with scope("slot"):
            wait_bytes(gath.at[number], g_slot.at[number])

    def own_rows(h, dc):
        with scope(f"wait_cache{h}"):
            wait_bytes(cache.at[h, pl.ds(0, nz - 1)], z_recv.at[4 + h])

        @pl.when(odd == 1)
        def _():
            fill(h).wait_recv()

        mine = jnp.where(odd == 1, theirs[h].astype(F32), 0.0)
        table = (cache[h].astype(F32) + mine).astype(BF16).reshape(ncodes, width)
        gath[0, h] = (aloc[h] + dot_nn(fw[h], table)).astype(BF16)
        for r, s in zip((*low, *high), (*high, *low), strict=True):
            send(h, r, (0, 0), right, dc)
            send(h, s, (0, 0), left, dc)
        for r in range(nch):
            send(h, r, (0, 0), 0, 1, True)

    def project(slot, first=False):
        number = slot[0] * 2 + slot[1]
        rows = jnp.concatenate([gath[number, h] for h in range(heads)], axis=1)
        add = dot_nn(rows, wcol[number])
        acc[...] = add if first else acc[...] + add

    def weights_in():
        with scope("wait_w"):
            own_w.wait()
            w_all = wcol.at[pl.ds(1, len(peers))]
            wait_bytes(w_all, w_recv)
            wait_bytes(w_all, w_send)

    @pl.when(c == 0)
    def _():
        for h in range(heads):
            own_rows(h, 1)
        weights_in()
        project((0, 0), True)
        for slot in ((0, 1), (left, 1), (right, 1), (beyond, 1), (left, 0), (right, 0), (beyond, 0)):
            landed_whole(slot)
            project(slot)
        out_ref[...] = acc[...].astype(BF16)
        wait_bytes(gath.at[pl.ds(0, 2)], g_send.at[0])
        wait_bytes(gath.at[0], g_send.at[1])

    @pl.when(c == 1)
    def _():
        def relay(h, sc):
            with scope(f"relay{h}{sc}"):
                for r, s in zip(low, high, strict=True):
                    landed(h, r, (left, sc))
                    send(h, r, (left, sc), right, 0)
                    send(h, r, (left, sc), 0, 1, True)
                    landed(h, s, (right, sc))
                    send(h, s, (right, sc), left, 0)
                    send(h, s, (right, sc), 0, 1, True)
                for r, s in zip(high, low, strict=True):
                    landed(h, r, (left, sc))
                    send(h, r, (left, sc), 0, 1, True)
                    landed(h, s, (right, sc))
                    send(h, s, (right, sc), 0, 1, True)

        def across(h, sc):
            with scope(f"across{h}{sc}"):
                for pair_of in zip(low, high, strict=True):
                    for r in pair_of:
                        landed(h, r, (beyond, sc))
                        send(h, r, (beyond, sc), 0, 1, True)

        own_rows(0, 0)
        own_rows(1, 0)
        weights_in()
        relay(0, 0)
        relay(1, 0)
        across(0, 0)
        project((0, 0), True)
        relay(0, 1)
        across(1, 0)
        project((left, 0))
        project((right, 0))
        relay(1, 1)
        across(0, 1)
        landed_whole((0, 1))
        project((0, 1))
        project((beyond, 0))
        across(1, 1)
        for slot in ((left, 1), (right, 1), (beyond, 1)):
            project(slot)
        out_ref[...] = acc[...].astype(BF16)
        wait_bytes(gath.at[pl.ds(0, 4)], g_send.at[0])
        wait_bytes(gath.at[pl.ds(0, 7)], g_send.at[1])

    with scope("tail"):
        for chunk, ref in ((0, csums), (3, csums), (4, cache.at[0]), (5, cache.at[1])):
            wait_bytes(ref.at[pl.ds(0, nz - 1)], z_send.at[chunk])
        for h in range(heads):
            wait_bytes(raw.at[h, pl.ds(0, npair - 1)], z_send.at[1 + h])
            swap(h).wait_send()

        @pl.when(odd == 0)
        def _():
            for h in range(heads):
                fill(h).wait_send()

        for chunk, source, target in (
            (0, ctot_s, ctot_r),
            (1, tot_s.at[0], tot_r.at[0]),
            (2, tot_s.at[1], tot_r.at[1]),
        ):
            for d in range(1, ny):

                @pl.when(y + d < ny)
                def _(chunk=chunk, source=source, target=target, d=d):
                    y_copy(source, target, chunk, d).wait_send()


def on_device(queries, values, codes, codebook, out_weight, *, ny, nz, nx):
    tokens, heads, width = queries.shape
    ncodes = codebook.shape[1]
    sl = ncodes // nz
    cols = out_weight.shape[1] // (nx * 2)
    depth = out_weight.shape[0]
    nch = 4
    anywhere = pl.BlockSpec(memory_space=pl.ANY)
    scratch = [
        pltpu.VMEM((tokens * heads, width), BF16),
        pltpu.VMEM((tokens * heads, width), BF16),
        pltpu.VMEM((heads, tokens), jnp.int32),
        pltpu.VMEM((heads, ncodes, width), BF16),
        pltpu.VMEM((tokens * heads, width), F32),
        pltpu.VMEM((heads, tokens, width), BF16),
        pltpu.VMEM((heads, tokens, width), BF16),
        pltpu.VMEM((heads, nz, sl, width), BF16),
        pltpu.VMEM((heads, nz, sl, width), BF16),
        pltpu.VMEM((heads, nz // 2, sl, width), BF16),
        pltpu.VMEM((heads, nz // 2, sl, width), BF16),
        pltpu.VMEM((heads, sl, width), BF16),
        pltpu.VMEM((heads, ny, sl, width), BF16),
        pltpu.VMEM((heads, nz // 2, sl, width), BF16),
        pltpu.VMEM((heads, nz, sl, width), BF16),
        pltpu.VMEM((nz, 1, width), F32),
        pltpu.VMEM((nz, 1, width), F32),
        pltpu.VMEM((1, width), F32),
        pltpu.VMEM((ny, 1, width), F32),
        pltpu.VMEM((nz, 1, width), F32),
        pltpu.VMEM((nz, 1, width), F32),
        pltpu.VMEM((heads, tokens, ncodes), F32),
        pltpu.VMEM((heads, tokens, ncodes), BF16),
        pltpu.VMEM((heads, tokens, width), F32),
        pltpu.VMEM((heads, 2, tokens, 1), F32),
        pltpu.VMEM((nx * 2, heads, tokens, width), BF16),
        pltpu.VMEM((nx * 2, depth, cols), BF16),
        pltpu.VMEM((tokens, cols), F32),
        pltpu.SemaphoreType.DMA((4,)),
        pltpu.SemaphoreType.DMA((10,)),
        pltpu.SemaphoreType.DMA((10,)),
        pltpu.SemaphoreType.DMA((3, ny - 1)),
        pltpu.SemaphoreType.DMA((3, ny - 1)),
        pltpu.SemaphoreType.DMA,
        pltpu.SemaphoreType.DMA,
        pltpu.SemaphoreType.DMA,
        pltpu.SemaphoreType.DMA((2,)),
        pltpu.SemaphoreType.DMA((nx * 2 - 2, heads, nch)),
        pltpu.SemaphoreType.DMA((nx * 2,)),
    ]
    return pl.pallas_call(
        functools.partial(kernel, ny=ny, nz=nz, nx=nx, nch=nch),
        out_shape=pltpu.VMEM((tokens, cols), BF16),
        in_specs=[anywhere] * 5,
        out_specs=pl.BlockSpec(memory_space=pltpu.VMEM),
        scratch_shapes=scratch,
        compiler_params=pltpu.CompilerParams(collective_id=0, has_side_effects=True),
        name="vq_layer",
    )(
        queries.reshape(tokens * heads, width),
        values.reshape(tokens * heads, width),
        codes.T,
        codebook,
        out_weight,
    )


def layer(mesh, ny, nz, nx):
    finer = Mesh(mesh.devices.reshape(ny, nz, nx, 2), ("y", "z", "x", "c"))
    placed = (
        P(CTX, HEAD, None),
        P(CTX, HEAD, None),
        P(CTX, HEAD),
        P(HEAD, None, None),
        P(HEAD, None),
    )
    return jax.shard_map(
        functools.partial(on_device, ny=ny, nz=nz, nx=nx),
        mesh=finer,
        in_specs=placed,
        out_specs=P(CTX, HEAD),
        check_vma=False,
    )


def solution(mesh):
    return layer(mesh, 4, 16, 4)
```

```python
import functools

import jax
import jax.numpy as jnp
from jax import lax
from jax.experimental import pallas as pl
from jax.experimental.pallas import tpu as pltpu
from jax.sharding import Mesh
from jax.sharding import PartitionSpec as P

MESH = pl.DeviceIdType.MESH
CTX = ("y", "z")
HEAD = ("x", "c")
F32 = jnp.float32
BF16 = jnp.bfloat16
NEG = float("-inf")


def dot_nt(a, b):
    return lax.dot_general(a, b, (((1,), (1,)), ((), ())), preferred_element_type=F32)


def dot_nn(a, b, precision=None):
    return lax.dot_general(
        a, b, (((1,), (0,)), ((), ())), precision=precision, preferred_element_type=F32
    )


def dot_tn(a, b):
    return lax.dot_general(a, b, (((0,), (0,)), ((), ())), preferred_element_type=F32)


def wait_bytes(ref, sem):
    pltpu.make_async_copy(ref, ref, sem).wait()


def kernel(
    q_ref, v_ref, row_ref, book_ref, w_ref, out_ref,
    qin, vin, codes, book, split, vals, qs,
    sums, theirs, gsum, raw, tot_s, tot_r, pre_s, cache,
    csums, craw, ctot_s, ctot_r, cpre_s, ccache,
    code_sc, fw, aloc, stat, gath, wcol, acc,
    in_sem, z_send, z_recv, y_send, y_recv, w_send, w_recv, w_local, g_send, g_recv, g_slot,
    *, ny, nz, nx, nch,
):
    heads, ncodes, width = book_ref.shape
    tokens = q_ref.shape[0] // heads
    sl = ncodes // nz
    part = tokens // nch
    cols = out_ref.shape[1]
    y, z, x, c = (lax.axis_index(name) for name in ("y", "z", "x", "c"))
    scope = jax.named_scope

    def far_first(j):
        step = (j + 1) // 2
        sign = 1 - 2 * lax.rem(j, 2)
        return lax.rem(z + nz // 2 + sign * step + nz, nz)

    def x_at(d):
        return lax.rem(x + d, nx)

    npair = nz // 2
    odd, pair = lax.rem(z, 2), z // 2
    partner = z + 1 - 2 * odd

    def slice_of(at):
        return lax.rem(at, 2) * npair + at // 2

    def far_pair(j):
        step = (j + 1) // 2
        sign = 1 - 2 * lax.rem(j, 2)
        return lax.rem(pair + npair // 2 + sign * step + npair, npair)

    barrier = pltpu.get_barrier_semaphore()

    def greet(j, carry):
        pl.semaphore_signal(barrier, inc=1, device_id={"z": far_first(j)}, device_id_type=MESH)
        return carry

    lax.fori_loop(0, nz - 1, greet, 0)
    for d in range(1, ny):
        there = {"y": lax.rem(y + d, ny)}
        pl.semaphore_signal(barrier, inc=1, device_id=there, device_id_type=MESH)
    peers = [(dx, dc) for dx in range(nx) for dc in range(2)][1:]
    for dx, dc in peers:
        there = {"x": x_at(dx), "c": lax.rem(c + dc, 2)}
        pl.semaphore_signal(barrier, inc=1, device_id=there, device_id_type=MESH)

    loads = []
    for number, (source, target) in enumerate(
        ((row_ref, codes), (v_ref, vin), (book_ref, book), (q_ref, qin))
    ):
        loads.append(pltpu.make_async_copy(source, target, in_sem.at[number]))
        loads[-1].start()

    with scope("load"):
        loads[0].wait()
        loads[1].wait()
    with scope("sums"):
        split[...] = vin[...].astype(F32)
        counts = None
        for h in range(heads):
            vals[h] = split[pl.ds(h, tokens, stride=heads), :].astype(BF16)
            onehot_t = (
                lax.broadcasted_iota(jnp.int32, (ncodes, tokens), 0) == codes[h : h + 1, :]
            ).astype(BF16)
            both = jnp.concatenate([vals[h], jnp.ones((tokens, width), BF16)], axis=1)
            summed = dot_nn(onehot_t, both)
            sums[h] = summed[:, :width].astype(BF16).reshape(nz, sl, width)
            lane = lax.broadcasted_iota(jnp.int32, (ncodes, width), 1)
            code = lax.broadcasted_iota(jnp.int32, (ncodes, width), 0)
            mine = jnp.where(lane == h * sl + lax.rem(code, sl), summed[:, width:], 0.0)
            counted = jnp.sum(mine.reshape(nz, sl, width), axis=1)
            counts = counted if counts is None else counts + counted
        csums[...] = counts.reshape(nz, 1, width)

    def block_scores(h):
        onehot_t = (
            lax.broadcasted_iota(jnp.int32, (ncodes, tokens), 0) == codes[h : h + 1, :]
        ).astype(BF16)
        keys_t = dot_tn(book[h], onehot_t).astype(BF16)
        scale = width ** (-0.5)
        code_sc[h] = dot_nt(qs[h], book[h]) * scale
        scores = dot_nn(qs[h], keys_t) * scale
        rows = lax.broadcasted_iota(jnp.int32, (tokens, tokens), 0)
        ends = lax.broadcasted_iota(jnp.int32, (tokens, tokens), 1)
        scores = jnp.where(rows >= ends, scores, NEG)
        top = jnp.max(scores, axis=1, keepdims=True)
        weights = jnp.exp(scores - top)
        aloc[h] = dot_nn(weights.astype(BF16), vals[h])
        stat[h, 0] = top
        stat[h, 1] = jnp.sum(weights, axis=1, keepdims=True)

    with scope("barrier"):
        pl.semaphore_wait(barrier, nz - 1 + ny - 1 + len(peers))

    def z_copy(source, target, chunk, there):
        return pltpu.make_async_remote_copy(
            src_ref=source,
            dst_ref=target,
            send_sem=z_send.at[chunk],
            recv_sem=z_recv.at[chunk],
            device_id={"z": there},
            device_id_type=MESH,
        )

    def push_counts():
        def push(j, carry):
            there = far_first(j)
            z_copy(csums.at[slice_of(there)], craw.at[z], 0, there).start()
            return carry

        lax.fori_loop(0, nz - 1, push, 0)
        craw[z] = csums[slice_of(z)]

    def push_counts_back():
        def push(j, carry):
            there = far_first(j)
            z_copy(cpre_s.at[there], ccache.at[slice_of(z)], 3, there).start()
            return carry

        lax.fori_loop(0, nz - 1, push, 0)
        ccache[slice_of(z)] = cpre_s[z]

    def push_pair_sums(h):
        def push(j, carry):
            there = far_pair(j)
            z_copy(gsum.at[h, there], raw.at[h, pair], 1 + h, 2 * there + odd).start()
            return carry

        lax.fori_loop(0, npair - 1, push, 0)
        raw[h, pair] = gsum[h, pair]

    def z_push_band(h, start, count):
        def push(j, carry):
            there = start + lax.rem(z + j, count)

            @pl.when(there != z)
            def _():
                z_copy(pre_s.at[h, there // 2], cache.at[h, slice_of(z)], 4 + h, there).start()

            return carry

        lax.fori_loop(0, count, push, 0)

    def half_rows(ref, h, which):
        return ref.at[h, pl.ds(which * npair, npair)]

    def swap(h):
        return z_copy(half_rows(sums, h, 1 - odd), half_rows(theirs, h, 1 - odd), 6 + h, partner)

    def fill(h):
        return z_copy(half_rows(sums, h, 0), half_rows(theirs, h, 0), 8 + h, partner)

    with scope("push_raw"):
        push_counts()
        for h in range(heads):
            swap(h).start()

    def w_slice(dx, dc):
        owner = x_at(dx) * 2 + lax.rem(c + dc, 2)
        return w_ref.at[:, pl.ds(pl.multiple_of(owner * cols, cols), cols)]

    own_w = pltpu.make_async_copy(w_slice(0, 0), wcol.at[0], w_local)
    own_w.start()
    for dx, dc in peers:
        pltpu.make_async_remote_copy(
            src_ref=w_slice(dx, dc),
            dst_ref=wcol.at[(nx - dx) % nx * 2 + dc],
            send_sem=w_send,
            recv_sem=w_recv,
            device_id={"x": x_at(dx), "c": lax.rem(c + dc, 2)},
            device_id_type=MESH,
        ).start()

    with scope("scores"):
        loads[2].wait()
        loads[3].wait()
        split[...] = qin[...].astype(F32)
        for h in range(heads):
            qs[h] = split[pl.ds(h, tokens, stride=heads), :].astype(BF16)
            block_scores(h)

    for h in range(heads):
        with scope(f"wait_swap{h}"):
            wait_bytes(half_rows(theirs, h, odd), z_recv.at[6 + h])
        own = half_rows(sums, h, odd)[...].astype(F32)
        gsum[h] = (own + half_rows(theirs, h, odd)[...].astype(F32)).astype(BF16)
        push_pair_sums(h)

    @pl.when(odd == 0)
    def _():
        for h in range(heads):
            fill(h).start()

    def y_copy(source, target, chunk, d):
        return pltpu.make_async_remote_copy(
            src_ref=source,
            dst_ref=target.at[d],
            send_sem=y_send.at[chunk, d - 1],
            recv_sem=y_recv.at[chunk, d - 1],
            device_id={"y": lax.rem(y + d, ny)},
            device_id_type=MESH,
        )

    def y_push(source, target, chunk):
        for d in range(1, ny):

            @pl.when(y + d < ny)
            def _(d=d):
                y_copy(source, target, chunk, d).start()

    with scope("wait_craw"):
        wait_bytes(craw.at[pl.ds(0, nz - 1)], z_recv.at[0])
    cbefore, so_far = [], jnp.zeros((1, width), F32)
    for n in range(nz):
        cbefore.append(so_far)
        so_far = so_far + craw[n]
    ctot_s[...] = so_far
    y_push(ctot_s, ctot_r, 0)
    def row_total(h):
        with scope(f"wait_raw{h}"):
            wait_bytes(raw.at[h, pl.ds(0, npair - 1)], z_recv.at[1 + h])
        so_far = raw[h, 0].astype(F32)
        for n in range(1, npair):
            so_far = so_far + raw[h, n].astype(F32)
        tot_s[h] = so_far.astype(BF16)
        y_push(tot_s.at[h], tot_r.at[h], 1 + h)

    def earlier_rows(source, target, chunk):
        total = None
        for d in range(1, ny):

            @pl.when(y >= d)
            def _(d=d):
                y_copy(source, target, chunk, d).wait_recv()

            row = jnp.where(y >= d, target[d].astype(F32), 0.0)
            total = row if total is None else total + row
        return total

    def send_prefix(h):
        with scope(f"wait_y{h}"):
            so_far = earlier_rows(tot_s.at[h], tot_r.at[h], 1 + h)
        with scope(f"prefix{h}"):
            for n in range(npair):
                pre_s[h, n] = so_far.astype(BF16)
                so_far = so_far + raw[h, n].astype(F32)
            cache[h, slice_of(z)] = pre_s[h, pair]
            z_push_band(h, 0, nz // 4)

    row_total(0)
    with scope("wait_cy"):
        above = earlier_rows(ctot_s, ctot_r, 0)
    for n in range(nz):
        cpre_s[n] = cbefore[n] + above
    push_counts_back()
    for h in range(1, heads):
        row_total(h)
    for h in range(heads):
        send_prefix(h)
    for start, count in ((nz // 4, nz // 4), (nz // 2, nz // 2)):
        for h in range(heads):
            z_push_band(h, start, count)

    with scope("wait_ccache"):
        wait_bytes(ccache.at[pl.ds(0, nz - 1)], z_recv.at[3])

    def code_weights(h):
        lane = lax.broadcasted_iota(jnp.int32, (width, ncodes), 0)
        code = lax.broadcasted_iota(jnp.int32, (width, ncodes), 1)
        pick = (lane == h * sl + lax.rem(code, sl)).astype(F32)
        spread = dot_nn(found, pick, lax.Precision.HIGHEST)
        group = lax.broadcasted_iota(jnp.int32, (nz, ncodes), 0)
        where = lax.broadcasted_iota(jnp.int32, (nz, ncodes), 1) // sl
        count = jnp.sum(jnp.where(group == where, spread, 0.0), axis=0, keepdims=True)
        scores = jnp.where(count > 0.0, code_sc[h], NEG)
        top = jnp.maximum(stat[h, 0], jnp.max(scores, axis=1, keepdims=True))
        weights = jnp.exp(scores - top)
        shift = jnp.exp(stat[h, 0] - top)
        den = stat[h, 1] * shift + jnp.sum(weights * count, axis=1, keepdims=True)
        inverse = 1.0 / den
        fw[h] = (weights * inverse).astype(BF16)
        aloc[h] = aloc[h] * (shift * inverse)

    with scope("weights"):
        found = ccache[...].reshape(nz, width)
        for h in range(heads):
            code_weights(h)

    right, left, beyond = 1, nx - 1, 2
    low, high = range(nch // 2), range(nch // 2, nch)

    def piece(slot, h, r):
        return gath.at[slot[0] * 2 + slot[1], h, pl.ds(r * part, part)]

    def send(h, r, slot, dx, dc, whole=False):
        there = ((slot[0] - dx) % nx, (slot[1] + dc) % 2)
        number = there[0] * 2 + there[1]
        pltpu.make_async_remote_copy(
            src_ref=piece(slot, h, r),
            dst_ref=piece(there, h, r),
            send_sem=g_send.at[0 if dx else 1],
            recv_sem=g_slot.at[number] if whole else g_recv.at[number - 2, h, r],
            device_id={"x": x_at(dx), "c": lax.rem(c + dc, 2)},
            device_id_type=MESH,
        ).start()

    def landed(h, r, slot):
        wait_bytes(piece(slot, h, r), g_recv.at[slot[0] * 2 + slot[1] - 2, h, r])

    def landed_whole(slot):
        number = slot[0] * 2 + slot[1]
        with scope("slot"):
            wait_bytes(gath.at[number], g_slot.at[number])

    def own_rows(h, dc):
        with scope(f"wait_cache{h}"):
            wait_bytes(cache.at[h, pl.ds(0, nz - 1)], z_recv.at[4 + h])

        @pl.when(odd == 1)
        def _():
            fill(h).wait_recv()

        mine = jnp.where(odd == 1, theirs[h].astype(F32), 0.0)
        table = (cache[h].astype(F32) + mine).astype(BF16).reshape(ncodes, width)
        gath[0, h] = (aloc[h] + dot_nn(fw[h], table)).astype(BF16)
        for r, s in zip((*low, *high), (*high, *low), strict=True):
            send(h, r, (0, 0), right, dc)
            send(h, s, (0, 0), left, dc)
        for r in range(nch):
            send(h, r, (0, 0), 0, 1, True)

    def project(slot, first=False):
        number = slot[0] * 2 + slot[1]
        rows = jnp.concatenate([gath[number, h] for h in range(heads)], axis=1)
        add = dot_nn(rows, wcol[number])
        acc[...] = add if first else acc[...] + add

    def weights_in():
        with scope("wait_w"):
            own_w.wait()
            w_all = wcol.at[pl.ds(1, len(peers))]
            wait_bytes(w_all, w_recv)
            wait_bytes(w_all, w_send)

    @pl.when(c == 0)
    def _():
        for h in range(heads):
            own_rows(h, 1)
        weights_in()
        project((0, 0), True)
        for slot in ((0, 1), (left, 1), (right, 1), (beyond, 1), (left, 0), (right, 0), (beyond, 0)):
            landed_whole(slot)
            project(slot)
        out_ref[...] = acc[...].astype(BF16)
        wait_bytes(gath.at[pl.ds(0, 2)], g_send.at[0])
        wait_bytes(gath.at[0], g_send.at[1])

    @pl.when(c == 1)
    def _():
        def relay(h, sc):
            with scope(f"relay{h}{sc}"):
                for r, s in zip(low, high, strict=True):
                    landed(h, r, (left, sc))
                    send(h, r, (left, sc), right, 0)
                    send(h, r, (left, sc), 0, 1, True)
                    landed(h, s, (right, sc))
                    send(h, s, (right, sc), left, 0)
                    send(h, s, (right, sc), 0, 1, True)
                for r, s in zip(high, low, strict=True):
                    landed(h, r, (left, sc))
                    send(h, r, (left, sc), 0, 1, True)
                    landed(h, s, (right, sc))
                    send(h, s, (right, sc), 0, 1, True)

        def across(h, sc):
            with scope(f"across{h}{sc}"):
                for pair_of in zip(low, high, strict=True):
                    for r in pair_of:
                        landed(h, r, (beyond, sc))
                        send(h, r, (beyond, sc), 0, 1, True)

        own_rows(0, 0)
        own_rows(1, 0)
        weights_in()
        relay(0, 0)
        relay(1, 0)
        across(0, 0)
        project((0, 0), True)
        relay(0, 1)
        across(1, 0)
        project((left, 0))
        project((right, 0))
        relay(1, 1)
        across(0, 1)
        landed_whole((0, 1))
        project((0, 1))
        project((beyond, 0))
        across(1, 1)
        for slot in ((left, 1), (right, 1), (beyond, 1)):
            project(slot)
        out_ref[...] = acc[...].astype(BF16)
        wait_bytes(gath.at[pl.ds(0, 4)], g_send.at[0])
        wait_bytes(gath.at[pl.ds(0, 7)], g_send.at[1])

    with scope("tail"):
        for chunk, ref in ((0, csums), (3, csums), (4, cache.at[0]), (5, cache.at[1])):
            wait_bytes(ref.at[pl.ds(0, nz - 1)], z_send.at[chunk])
        for h in range(heads):
            wait_bytes(raw.at[h, pl.ds(0, npair - 1)], z_send.at[1 + h])
            swap(h).wait_send()

        @pl.when(odd == 0)
        def _():
            for h in range(heads):
                fill(h).wait_send()

        for chunk, source, target in (
            (0, ctot_s, ctot_r),
            (1, tot_s.at[0], tot_r.at[0]),
            (2, tot_s.at[1], tot_r.at[1]),
        ):
            for d in range(1, ny):

                @pl.when(y + d < ny)
                def _(chunk=chunk, source=source, target=target, d=d):
                    y_copy(source, target, chunk, d).wait_send()


def on_device(queries, values, codes, codebook, out_weight, *, ny, nz, nx):
    tokens, heads, width = queries.shape
    ncodes = codebook.shape[1]
    sl = ncodes // nz
    cols = out_weight.shape[1] // (nx * 2)
    depth = out_weight.shape[0]
    nch = 4
    anywhere = pl.BlockSpec(memory_space=pl.ANY)
    scratch = [
        pltpu.VMEM((tokens * heads, width), BF16),
        pltpu.VMEM((tokens * heads, width), BF16),
        pltpu.VMEM((heads, tokens), jnp.int32),
        pltpu.VMEM((heads, ncodes, width), BF16),
        pltpu.VMEM((tokens * heads, width), F32),
        pltpu.VMEM((heads, tokens, width), BF16),
        pltpu.VMEM((heads, tokens, width), BF16),
        pltpu.VMEM((heads, nz, sl, width), BF16),
        pltpu.VMEM((heads, nz, sl, width), BF16),
        pltpu.VMEM((heads, nz // 2, sl, width), BF16),
        pltpu.VMEM((heads, nz // 2, sl, width), BF16),
        pltpu.VMEM((heads, sl, width), BF16),
        pltpu.VMEM((heads, ny, sl, width), BF16),
        pltpu.VMEM((heads, nz // 2, sl, width), BF16),
        pltpu.VMEM((heads, nz, sl, width), BF16),
        pltpu.VMEM((nz, 1, width), F32),
        pltpu.VMEM((nz, 1, width), F32),
        pltpu.VMEM((1, width), F32),
        pltpu.VMEM((ny, 1, width), F32),
        pltpu.VMEM((nz, 1, width), F32),
        pltpu.VMEM((nz, 1, width), F32),
        pltpu.VMEM((heads, tokens, ncodes), F32),
        pltpu.VMEM((heads, tokens, ncodes), BF16),
        pltpu.VMEM((heads, tokens, width), F32),
        pltpu.VMEM((heads, 2, tokens, 1), F32),
        pltpu.VMEM((nx * 2, heads, tokens, width), BF16),
        pltpu.VMEM((nx * 2, depth, cols), BF16),
        pltpu.VMEM((tokens, cols), F32),
        pltpu.SemaphoreType.DMA((4,)),
        pltpu.SemaphoreType.DMA((10,)),
        pltpu.SemaphoreType.DMA((10,)),
        pltpu.SemaphoreType.DMA((3, ny - 1)),
        pltpu.SemaphoreType.DMA((3, ny - 1)),
        pltpu.SemaphoreType.DMA,
        pltpu.SemaphoreType.DMA,
        pltpu.SemaphoreType.DMA,
        pltpu.SemaphoreType.DMA((2,)),
        pltpu.SemaphoreType.DMA((nx * 2 - 2, heads, nch)),
        pltpu.SemaphoreType.DMA((nx * 2,)),
    ]
    return pl.pallas_call(
        functools.partial(kernel, ny=ny, nz=nz, nx=nx, nch=nch),
        out_shape=pltpu.VMEM((tokens, cols), BF16),
        in_specs=[anywhere] * 5,
        out_specs=pl.BlockSpec(memory_space=pltpu.VMEM),
        scratch_shapes=scratch,
        compiler_params=pltpu.CompilerParams(collective_id=0, has_side_effects=True),
        name="vq_layer",
    )(
        queries.reshape(tokens * heads, width),
        values.reshape(tokens * heads, width),
        codes.T,
        codebook,
        out_weight,
    )


def layer(mesh, ny, nz, nx):
    finer = Mesh(mesh.devices.reshape(ny, nz, nx, 2), ("y", "z", "x", "c"))
    placed = (
        P(CTX, HEAD, None),
        P(CTX, HEAD, None),
        P(CTX, HEAD),
        P(HEAD, None, None),
        P(HEAD, None),
    )
    return jax.shard_map(
        functools.partial(on_device, ny=ny, nz=nz, nx=nx),
        mesh=finer,
        in_specs=placed,
        out_specs=P(CTX, HEAD),
        check_vma=False,
    )


def solution(mesh):
    return layer(mesh, 4, 16, 4)
```

```python
import functools

import jax
import jax.numpy as jnp
from jax import lax
from jax.experimental import pallas as pl
from jax.experimental.pallas import tpu as pltpu
from jax.sharding import Mesh
from jax.sharding import PartitionSpec as P

MESH = pl.DeviceIdType.MESH
CTX = ("y", "z")
HEAD = ("x", "c")
F32 = jnp.float32
BF16 = jnp.bfloat16
NEG = float("-inf")


def dot_nt(a, b):
    return lax.dot_general(a, b, (((1,), (1,)), ((), ())), preferred_element_type=F32)


def dot_nn(a, b, precision=None):
    return lax.dot_general(
        a, b, (((1,), (0,)), ((), ())), precision=precision, preferred_element_type=F32
    )


def dot_tn(a, b):
    return lax.dot_general(a, b, (((0,), (0,)), ((), ())), preferred_element_type=F32)


def wait_bytes(ref, sem):
    pltpu.make_async_copy(ref, ref, sem).wait()


def kernel(
    q_ref, v_ref, row_ref, book_ref, w_ref, out_ref,
    qin, vin, codes, book, split, vals, qs,
    sums, theirs, gsum, raw, tot_s, tot_r, pre_s, cache,
    csums, craw, ctot_s, ctot_r, cpre_s, ccache,
    code_sc, fw, aloc, stat, gath, wcol, acc,
    in_sem, z_send, z_recv, y_send, y_recv, w_send, w_recv, w_local, g_send, g_recv, g_slot,
    *, ny, nz, nx, nch,
):
    heads, ncodes, width = book_ref.shape
    tokens = q_ref.shape[0] // heads
    sl = ncodes // nz
    part = tokens // nch
    cols = out_ref.shape[1]
    y, z, x, c = (lax.axis_index(name) for name in ("y", "z", "x", "c"))
    scope = jax.named_scope

    def far_first(j):
        step = (j + 1) // 2
        sign = 1 - 2 * lax.rem(j, 2)
        return lax.rem(z + nz // 2 + sign * step + nz, nz)

    def x_at(d):
        return lax.rem(x + d, nx)

    npair = nz // 2
    odd, pair = lax.rem(z, 2), z // 2
    partner = z + 1 - 2 * odd

    def slice_of(at):
        return lax.rem(at, 2) * npair + at // 2

    def far_pair(j):
        step = (j + 1) // 2
        sign = 1 - 2 * lax.rem(j, 2)
        return lax.rem(pair + npair // 2 + sign * step + npair, npair)

    barrier = pltpu.get_barrier_semaphore()

    def greet(j, carry):
        pl.semaphore_signal(barrier, inc=1, device_id={"z": far_first(j)}, device_id_type=MESH)
        return carry

    lax.fori_loop(0, nz - 1, greet, 0)
    for d in range(1, ny):
        there = {"y": lax.rem(y + d, ny)}
        pl.semaphore_signal(barrier, inc=1, device_id=there, device_id_type=MESH)
    peers = [(dx, dc) for dx in range(nx) for dc in range(2)][1:]
    for dx, dc in peers:
        there = {"x": x_at(dx), "c": lax.rem(c + dc, 2)}
        pl.semaphore_signal(barrier, inc=1, device_id=there, device_id_type=MESH)

    loads = []
    for number, (source, target) in enumerate(
        ((row_ref, codes), (v_ref, vin), (book_ref, book), (q_ref, qin))
    ):
        loads.append(pltpu.make_async_copy(source, target, in_sem.at[number]))
        loads[-1].start()

    with scope("load"):
        loads[0].wait()
        loads[1].wait()
    with scope("sums"):
        split[...] = vin[...].astype(F32)
        counts = None
        for h in range(heads):
            vals[h] = split[pl.ds(h, tokens, stride=heads), :].astype(BF16)
            onehot_t = (
                lax.broadcasted_iota(jnp.int32, (ncodes, tokens), 0) == codes[h : h + 1, :]
            ).astype(BF16)
            both = jnp.concatenate([vals[h], jnp.ones((tokens, width), BF16)], axis=1)
            summed = dot_nn(onehot_t, both)
            sums[h] = summed[:, :width].astype(BF16).reshape(nz, sl, width)
            lane = lax.broadcasted_iota(jnp.int32, (ncodes, width), 1)
            code = lax.broadcasted_iota(jnp.int32, (ncodes, width), 0)
            mine = jnp.where(lane == h * sl + lax.rem(code, sl), summed[:, width:], 0.0)
            counted = jnp.sum(mine.reshape(nz, sl, width), axis=1)
            counts = counted if counts is None else counts + counted
        csums[...] = counts.reshape(nz, 1, width)

    def block_scores(h):
        onehot_t = (
            lax.broadcasted_iota(jnp.int32, (ncodes, tokens), 0) == codes[h : h + 1, :]
        ).astype(BF16)
        keys_t = dot_tn(book[h], onehot_t).astype(BF16)
        scale = width ** (-0.5)
        code_sc[h] = dot_nt(qs[h], book[h]) * scale
        scores = dot_nn(qs[h], keys_t) * scale
        rows = lax.broadcasted_iota(jnp.int32, (tokens, tokens), 0)
        ends = lax.broadcasted_iota(jnp.int32, (tokens, tokens), 1)
        scores = jnp.where(rows >= ends, scores, NEG)
        top = jnp.max(scores, axis=1, keepdims=True)
        weights = jnp.exp(scores - top)
        aloc[h] = dot_nn(weights.astype(BF16), vals[h])
        stat[h, 0] = top
        stat[h, 1] = jnp.sum(weights, axis=1, keepdims=True)

    with scope("barrier"):
        pl.semaphore_wait(barrier, nz - 1 + ny - 1 + len(peers))

    def z_copy(source, target, chunk, there):
        return pltpu.make_async_remote_copy(
            src_ref=source,
            dst_ref=target,
            send_sem=z_send.at[chunk],
            recv_sem=z_recv.at[chunk],
            device_id={"z": there},
            device_id_type=MESH,
        )

    def push_counts():
        def push(j, carry):
            there = far_first(j)
            z_copy(csums.at[slice_of(there)], craw.at[z], 0, there).start()
            return carry

        lax.fori_loop(0, nz - 1, push, 0)
        craw[z] = csums[slice_of(z)]

    def push_counts_back():
        def push(j, carry):
            there = far_first(j)
            z_copy(cpre_s.at[there], ccache.at[slice_of(z)], 3, there).start()
            return carry

        lax.fori_loop(0, nz - 1, push, 0)
        ccache[slice_of(z)] = cpre_s[z]

    def push_pair_sums(h):
        def push(j, carry):
            there = far_pair(j)
            z_copy(gsum.at[h, there], raw.at[h, pair], 1 + h, 2 * there + odd).start()
            return carry

        lax.fori_loop(0, npair - 1, push, 0)
        raw[h, pair] = gsum[h, pair]

    def z_push_band(h, start, count):
        def push(j, carry):
            there = start + lax.rem(z + j, count)

            @pl.when(there != z)
            def _():
                z_copy(pre_s.at[h, there // 2], cache.at[h, slice_of(z)], 4 + h, there).start()

            return carry

        lax.fori_loop(0, count, push, 0)

    def half_rows(ref, h, which):
        return ref.at[h, pl.ds(which * npair, npair)]

    def swap(h):
        return z_copy(half_rows(sums, h, 1 - odd), half_rows(theirs, h, 1 - odd), 6 + h, partner)

    def fill(h):
        return z_copy(half_rows(sums, h, 0), half_rows(theirs, h, 0), 8 + h, partner)

    with scope("push_raw"):
        push_counts()
        for h in range(heads):
            swap(h).start()

    def w_slice(dx, dc):
        owner = x_at(dx) * 2 + lax.rem(c + dc, 2)
        return w_ref.at[:, pl.ds(pl.multiple_of(owner * cols, cols), cols)]

    own_w = pltpu.make_async_copy(w_slice(0, 0), wcol.at[0], w_local)
    own_w.start()
    for dx, dc in peers:
        pltpu.make_async_remote_copy(
            src_ref=w_slice(dx, dc),
            dst_ref=wcol.at[(nx - dx) % nx * 2 + dc],
            send_sem=w_send,
            recv_sem=w_recv,
            device_id={"x": x_at(dx), "c": lax.rem(c + dc, 2)},
            device_id_type=MESH,
        ).start()

    with scope("scores"):
        loads[2].wait()
        loads[3].wait()
        split[...] = qin[...].astype(F32)
        for h in range(heads):
            qs[h] = split[pl.ds(h, tokens, stride=heads), :].astype(BF16)
            block_scores(h)

    for h in range(heads):
        with scope(f"wait_swap{h}"):
            wait_bytes(half_rows(theirs, h, odd), z_recv.at[6 + h])
        own = half_rows(sums, h, odd)[...].astype(F32)
        gsum[h] = (own + half_rows(theirs, h, odd)[...].astype(F32)).astype(BF16)
        push_pair_sums(h)

    @pl.when(odd == 0)
    def _():
        for h in range(heads):
            fill(h).start()

    def y_copy(source, target, chunk, d):
        return pltpu.make_async_remote_copy(
            src_ref=source,
            dst_ref=target.at[d],
            send_sem=y_send.at[chunk, d - 1],
            recv_sem=y_recv.at[chunk, d - 1],
            device_id={"y": lax.rem(y + d, ny)},
            device_id_type=MESH,
        )

    def y_push(source, target, chunk):
        for d in range(1, ny):

            @pl.when(y + d < ny)
            def _(d=d):
                y_copy(source, target, chunk, d).start()

    with scope("wait_craw"):
        wait_bytes(craw.at[pl.ds(0, nz - 1)], z_recv.at[0])
    cbefore, so_far = [], jnp.zeros((1, width), F32)
    for n in range(nz):
        cbefore.append(so_far)
        so_far = so_far + craw[n]
    ctot_s[...] = so_far
    y_push(ctot_s, ctot_r, 0)
    def row_total(h):
        with scope(f"wait_raw{h}"):
            wait_bytes(raw.at[h, pl.ds(0, npair - 1)], z_recv.at[1 + h])
        so_far = raw[h, 0].astype(F32)
        for n in range(1, npair):
            so_far = so_far + raw[h, n].astype(F32)
        tot_s[h] = so_far.astype(BF16)
        y_push(tot_s.at[h], tot_r.at[h], 1 + h)

    def earlier_rows(source, target, chunk):
        total = None
        for d in range(1, ny):

            @pl.when(y >= d)
            def _(d=d):
                y_copy(source, target, chunk, d).wait_recv()

            row = jnp.where(y >= d, target[d].astype(F32), 0.0)
            total = row if total is None else total + row
        return total

    def send_prefix(h):
        with scope(f"wait_y{h}"):
            so_far = earlier_rows(tot_s.at[h], tot_r.at[h], 1 + h)
        with scope(f"prefix{h}"):
            for n in range(npair):
                pre_s[h, n] = so_far.astype(BF16)
                so_far = so_far + raw[h, n].astype(F32)
            cache[h, slice_of(z)] = pre_s[h, pair]
            z_push_band(h, 0, nz // 4)

    row_total(0)
    with scope("wait_cy"):
        above = earlier_rows(ctot_s, ctot_r, 0)
    for n in range(nz):
        cpre_s[n] = cbefore[n] + above
    push_counts_back()
    for h in range(1, heads):
        row_total(h)
    for h in range(heads):
        send_prefix(h)
    for start, count in ((nz // 4, nz // 4), (nz // 2, nz // 2)):
        for h in range(heads):
            z_push_band(h, start, count)

    with scope("wait_ccache"):
        wait_bytes(ccache.at[pl.ds(0, nz - 1)], z_recv.at[3])

    def code_weights(h):
        lane = lax.broadcasted_iota(jnp.int32, (width, ncodes), 0)
        code = lax.broadcasted_iota(jnp.int32, (width, ncodes), 1)
        pick = (lane == h * sl + lax.rem(code, sl)).astype(F32)
        spread = dot_nn(found, pick, lax.Precision.HIGHEST)
        group = lax.broadcasted_iota(jnp.int32, (nz, ncodes), 0)
        where = lax.broadcasted_iota(jnp.int32, (nz, ncodes), 1) // sl
        count = jnp.sum(jnp.where(group == where, spread, 0.0), axis=0, keepdims=True)
        scores = jnp.where(count > 0.0, code_sc[h], NEG)
        top = jnp.maximum(stat[h, 0], jnp.max(scores, axis=1, keepdims=True))
        weights = jnp.exp(scores - top)
        shift = jnp.exp(stat[h, 0] - top)
        den = stat[h, 1] * shift + jnp.sum(weights * count, axis=1, keepdims=True)
        inverse = 1.0 / den
        fw[h] = (weights * inverse).astype(BF16)
        aloc[h] = aloc[h] * (shift * inverse)

    with scope("weights"):
        found = ccache[...].reshape(nz, width)
        for h in range(heads):
            code_weights(h)

    right, left, beyond = 1, nx - 1, 2
    low, high = range(nch // 2), range(nch // 2, nch)

    def piece(slot, h, r):
        return gath.at[slot[0] * 2 + slot[1], h, pl.ds(r * part, part)]

    def send(h, r, slot, dx, dc, whole=False):
        there = ((slot[0] - dx) % nx, (slot[1] + dc) % 2)
        number = there[0] * 2 + there[1]
        pltpu.make_async_remote_copy(
            src_ref=piece(slot, h, r),
            dst_ref=piece(there, h, r),
            send_sem=g_send.at[0 if dx else 1],
            recv_sem=g_slot.at[number] if whole else g_recv.at[number - 2, h, r],
            device_id={"x": x_at(dx), "c": lax.rem(c + dc, 2)},
            device_id_type=MESH,
        ).start()

    def landed(h, r, slot):
        wait_bytes(piece(slot, h, r), g_recv.at[slot[0] * 2 + slot[1] - 2, h, r])

    def landed_whole(slot):
        number = slot[0] * 2 + slot[1]
        with scope("slot"):
            wait_bytes(gath.at[number], g_slot.at[number])

    def own_rows(h, dc):
        with scope(f"wait_cache{h}"):
            wait_bytes(cache.at[h, pl.ds(0, nz - 1)], z_recv.at[4 + h])

        @pl.when(odd == 1)
        def _():
            fill(h).wait_recv()

        mine = jnp.where(odd == 1, theirs[h].astype(F32), 0.0)
        table = (cache[h].astype(F32) + mine).astype(BF16).reshape(ncodes, width)
        gath[0, h] = (aloc[h] + dot_nn(fw[h], table)).astype(BF16)
        for r, s in zip((*low, *high), (*high, *low), strict=True):
            send(h, r, (0, 0), right, dc)
            send(h, s, (0, 0), left, dc)
        for r in range(nch):
            send(h, r, (0, 0), 0, 1, True)

    def project(slot, first=False):
        number = slot[0] * 2 + slot[1]
        rows = jnp.concatenate([gath[number, h] for h in range(heads)], axis=1)
        add = dot_nn(rows, wcol[number])
        acc[...] = add if first else acc[...] + add

    def weights_in():
        with scope("wait_w"):
            own_w.wait()
            w_all = wcol.at[pl.ds(1, len(peers))]
            wait_bytes(w_all, w_recv)
            wait_bytes(w_all, w_send)

    @pl.when(c == 0)
    def _():
        for h in range(heads):
            own_rows(h, 1)
        weights_in()
        project((0, 0), True)
        for slot in ((0, 1), (left, 1), (right, 1), (beyond, 1), (left, 0), (right, 0), (beyond, 0)):
            landed_whole(slot)
            project(slot)
        out_ref[...] = acc[...].astype(BF16)
        wait_bytes(gath.at[pl.ds(0, 2)], g_send.at[0])
        wait_bytes(gath.at[0], g_send.at[1])

    @pl.when(c == 1)
    def _():
        def relay(h, sc):
            with scope(f"relay{h}{sc}"):
                for r, s in zip(low, high, strict=True):
                    landed(h, r, (left, sc))
                    send(h, r, (left, sc), right, 0)
                    send(h, r, (left, sc), 0, 1, True)
                    landed(h, s, (right, sc))
                    send(h, s, (right, sc), left, 0)
                    send(h, s, (right, sc), 0, 1, True)
                for r, s in zip(high, low, strict=True):
                    landed(h, r, (left, sc))
                    send(h, r, (left, sc), 0, 1, True)
                    landed(h, s, (right, sc))
                    send(h, s, (right, sc), 0, 1, True)

        def across(h, sc):
            with scope(f"across{h}{sc}"):
                for pair_of in zip(low, high, strict=True):
                    for r in pair_of:
                        landed(h, r, (beyond, sc))
                        send(h, r, (beyond, sc), 0, 1, True)

        own_rows(0, 0)
        own_rows(1, 0)
        weights_in()
        relay(0, 0)
        relay(1, 0)
        across(0, 0)
        project((0, 0), True)
        relay(0, 1)
        across(1, 0)
        project((left, 0))
        project((right, 0))
        relay(1, 1)
        across(0, 1)
        landed_whole((0, 1))
        project((0, 1))
        for slot in ((beyond, 0), (left, 1), (right, 1)):
            project(slot)
        across(1, 1)
        project((beyond, 1))
        out_ref[...] = acc[...].astype(BF16)
        wait_bytes(gath.at[pl.ds(0, 4)], g_send.at[0])
        wait_bytes(gath.at[pl.ds(0, 7)], g_send.at[1])

    with scope("tail"):
        for chunk, ref in ((0, csums), (3, csums), (4, cache.at[0]), (5, cache.at[1])):
            wait_bytes(ref.at[pl.ds(0, nz - 1)], z_send.at[chunk])
        for h in range(heads):
            wait_bytes(raw.at[h, pl.ds(0, npair - 1)], z_send.at[1 + h])
            swap(h).wait_send()

        @pl.when(odd == 0)
        def _():
            for h in range(heads):
                fill(h).wait_send()

        for chunk, source, target in (
            (0, ctot_s, ctot_r),
            (1, tot_s.at[0], tot_r.at[0]),
            (2, tot_s.at[1], tot_r.at[1]),
        ):
            for d in range(1, ny):

                @pl.when(y + d < ny)
                def _(chunk=chunk, source=source, target=target, d=d):
                    y_copy(source, target, chunk, d).wait_send()


def on_device(queries, values, codes, codebook, out_weight, *, ny, nz, nx):
    tokens, heads, width = queries.shape
    ncodes = codebook.shape[1]
    sl = ncodes // nz
    cols = out_weight.shape[1] // (nx * 2)
    depth = out_weight.shape[0]
    nch = 4
    anywhere = pl.BlockSpec(memory_space=pl.ANY)
    scratch = [
        pltpu.VMEM((tokens * heads, width), BF16),
        pltpu.VMEM((tokens * heads, width), BF16),
        pltpu.VMEM((heads, tokens), jnp.int32),
        pltpu.VMEM((heads, ncodes, width), BF16),
        pltpu.VMEM((tokens * heads, width), F32),
        pltpu.VMEM((heads, tokens, width), BF16),
        pltpu.VMEM((heads, tokens, width), BF16),
        pltpu.VMEM((heads, nz, sl, width), BF16),
        pltpu.VMEM((heads, nz, sl, width), BF16),
        pltpu.VMEM((heads, nz // 2, sl, width), BF16),
        pltpu.VMEM((heads, nz // 2, sl, width), BF16),
        pltpu.VMEM((heads, sl, width), BF16),
        pltpu.VMEM((heads, ny, sl, width), BF16),
        pltpu.VMEM((heads, nz // 2, sl, width), BF16),
        pltpu.VMEM((heads, nz, sl, width), BF16),
        pltpu.VMEM((nz, 1, width), F32),
        pltpu.VMEM((nz, 1, width), F32),
        pltpu.VMEM((1, width), F32),
        pltpu.VMEM((ny, 1, width), F32),
        pltpu.VMEM((nz, 1, width), F32),
        pltpu.VMEM((nz, 1, width), F32),
        pltpu.VMEM((heads, tokens, ncodes), F32),
        pltpu.VMEM((heads, tokens, ncodes), BF16),
        pltpu.VMEM((heads, tokens, width), F32),
        pltpu.VMEM((heads, 2, tokens, 1), F32),
        pltpu.VMEM((nx * 2, heads, tokens, width), BF16),
        pltpu.VMEM((nx * 2, depth, cols), BF16),
        pltpu.VMEM((tokens, cols), F32),
        pltpu.SemaphoreType.DMA((4,)),
        pltpu.SemaphoreType.DMA((10,)),
        pltpu.SemaphoreType.DMA((10,)),
        pltpu.SemaphoreType.DMA((3, ny - 1)),
        pltpu.SemaphoreType.DMA((3, ny - 1)),
        pltpu.SemaphoreType.DMA,
        pltpu.SemaphoreType.DMA,
        pltpu.SemaphoreType.DMA,
        pltpu.SemaphoreType.DMA((2,)),
        pltpu.SemaphoreType.DMA((nx * 2 - 2, heads, nch)),
        pltpu.SemaphoreType.DMA((nx * 2,)),
    ]
    return pl.pallas_call(
        functools.partial(kernel, ny=ny, nz=nz, nx=nx, nch=nch),
        out_shape=pltpu.VMEM((tokens, cols), BF16),
        in_specs=[anywhere] * 5,
        out_specs=pl.BlockSpec(memory_space=pltpu.VMEM),
        scratch_shapes=scratch,
        compiler_params=pltpu.CompilerParams(collective_id=0, has_side_effects=True),
        name="vq_layer",
    )(
        queries.reshape(tokens * heads, width),
        values.reshape(tokens * heads, width),
        codes.T,
        codebook,
        out_weight,
    )


def layer(mesh, ny, nz, nx):
    finer = Mesh(mesh.devices.reshape(ny, nz, nx, 2), ("y", "z", "x", "c"))
    placed = (
        P(CTX, HEAD, None),
        P(CTX, HEAD, None),
        P(CTX, HEAD),
        P(HEAD, None, None),
        P(HEAD, None),
    )
    return jax.shard_map(
        functools.partial(on_device, ny=ny, nz=nz, nx=nx),
        mesh=finer,
        in_specs=placed,
        out_specs=P(CTX, HEAD),
        check_vma=False,
    )


def solution(mesh):
    return layer(mesh, 4, 16, 4)
```
